32 devices in a mesh: seq: 8 (over z, y), head: 4 (over x, core).
Axes of the slice: x: 2, y: 2, z: 4, core: 2. Of those that a mesh axis runs over, the one named last changes fastest.
Arguments:
- queries: bfloat16 [4096, 12288], P(('seq', 'head')), may hold values from -8 to 8
- latent: bfloat16 [4096, 512], P(('seq', 'head')), may hold values from -6 to 6
- rope_keys: bfloat16 [4096, 64], P(('seq', 'head')), may hold values from -8 to 8
- key_weight: bfloat16 [512, 8192], P('seq', 'head'), may hold values from -0.25 to 0.25
- value_weight: bfloat16 [512, 8192], P('seq', 'head'), may hold values from -0.25 to 0.25
- doc_lengths: int32 [32], replicated, may hold values from 1 to 254, as said below
Outputs:
- attended: bfloat16 [4096, 8192], P(('seq', 'head'))
The draws below stay inside these ranges and needn't reach their ends.
Inputs may be any that keep to these rules, and one draw needn't show every extreme that they name: `doc_lengths`: the documents lie in order in the pack and their lengths sum to 4096; document 0 starts at position 0 and every other document d starts strictly inside positions d * 128 to (d + 1) * 128 - 1, excluding the first of these; one length is exactly 254.
All inputs are finite; a program needn't handle non-finite values.
Results may differ from the reference program's by a relative error of at most 0.0062.
Values may be sent and summed in bfloat16 or wider, within the bound.
A program may use at most 128 MiB of HBM per device.

```python
import math
import jax
import jax.numpy as jnp
from jax import lax

KV_RANK = 512
NOPE = 128
ROPE = 64
VDIM = 128
HEADS = 64
TOK_DEV = 128
TOKENS = 4096
DOCS = 32
N_HEAD = 4


def draw_queries(key, part):
    shape = (TOKENS, HEADS, NOPE + ROPE)
    own_key = jax.random.fold_in(key, 11)
    drawn = jnp.clip(2.0 * jax.random.normal(own_key, shape, jnp.float32), -8.0, 8.0)
    return drawn.reshape(TOKENS, HEADS * (NOPE + ROPE)).astype(jnp.bfloat16)


def draw_rope_keys(key, part):
    shape = (TOKENS, ROPE)
    own_key = jax.random.fold_in(key, 12)
    drawn = jnp.clip(jax.random.normal(own_key, shape, jnp.float32), -8.0, 8.0)
    return drawn.astype(jnp.bfloat16)


def draw_doc_lengths(key, part):
    slot_rows = TOKENS // DOCS
    jitter = jax.random.randint(jax.random.fold_in(key, 21), (DOCS,), 1, slot_rows)
    chosen = jax.random.randint(jax.random.fold_in(key, 22), (), 1, DOCS - 1)
    index = jnp.arange(DOCS, dtype=jnp.int32)
    jitter = jnp.where(index == 1, jnp.minimum(jitter, slot_rows - 2), jitter)
    jitter = jnp.where(index == chosen, 1, jitter)
    jitter = jnp.where(index == chosen + 1, slot_rows - 1, jitter)
    jitter = jnp.where(index == 0, 0, jitter)
    starts = index * slot_rows + jitter
    ends = jnp.concatenate([starts[1:], jnp.full((1,), TOKENS, jnp.int32)])
    return (ends - starts).astype(jnp.int32)


def steps_of(key, dims, cuts, low, high):
    factor_of, own = 1.0, jax.random.fold_in(key, 6)
    for position, shards_of in cuts:
        heights = jnp.exp(jax.random.uniform(jax.random.fold_in(own, position), (shards_of,), jnp.float32, low / len(cuts), high / len(cuts)))
        factor_of = factor_of * jnp.repeat(heights, dims[position] // shards_of).reshape([-1 if axis == position else 1 for axis in range(len(dims))])
    return factor_of


def scatter_about(stream_key, extent, spread, bound, pieces=(), held_as=jnp.bfloat16):
    array = spread * jax.random.normal(stream_key, extent, jnp.float32)
    if pieces:
        array = array * steps_of(stream_key, extent, pieces, -0.22, 0.18)
    return jnp.clip(array, -bound, bound).astype(held_as)


def setup_inputs(seed: int = 0) -> dict:
    key_of = jax.random.split(jax.random.key(seed), 7)
    queries = draw_queries(jax.random.fold_in(key_of[6], 71), 0)
    latent = scatter_about(key_of[1], (TOKENS, KV_RANK), 1.0, 6.0, ((0, 32),))
    rope_keys = draw_rope_keys(jax.random.fold_in(key_of[6], 71), 0)
    key_weight = scatter_about(key_of[3], (KV_RANK, HEADS * NOPE), KV_RANK ** -0.5, 0.25, ((0, 8), (1, 4)))
    value_weight = scatter_about(key_of[4], (KV_RANK, HEADS * VDIM), KV_RANK ** -0.5, 0.25, ((0, 8), (1, 4)))
    doc_lengths = draw_doc_lengths(jax.random.fold_in(key_of[6], 71), 0)
    return dict(queries=queries, latent=latent, rope_keys=rope_keys, key_weight=key_weight, value_weight=value_weight, doc_lengths=doc_lengths)


def reference(queries, latent, rope_keys, key_weight, value_weight, doc_lengths):
    total_rows = queries.shape[0]
    group_rows = TOK_DEV * N_HEAD
    block_rows = min(512, group_rows)
    qk_width = NOPE + ROPE
    key_span = group_rows + block_rows
    score_scale = 1.0 / math.sqrt(qk_width)
    starts = (jnp.cumsum(doc_lengths) - doc_lengths).astype(jnp.int32)
    places = jnp.arange(total_rows, dtype=jnp.int32)
    started = (starts[None, :] <= places[:, None]).astype(jnp.int32)
    doc_of = (lax.optimization_barrier(jnp.sum(started, axis=1)) - 1).astype(jnp.int32)
    keys = jnp.dot(latent, key_weight, preferred_element_type=jnp.float32).astype(jnp.bfloat16)
    values = jnp.dot(latent, value_weight, preferred_element_type=jnp.float32).astype(jnp.bfloat16)
    keys_front = jnp.concatenate([jnp.zeros((group_rows, keys.shape[1]), jnp.bfloat16), keys], axis=0)
    values_front = jnp.concatenate([jnp.zeros((group_rows, values.shape[1]), jnp.bfloat16), values], axis=0)
    rope_front = jnp.concatenate([jnp.zeros((group_rows, ROPE), jnp.bfloat16), rope_keys], axis=0)
    docs_front = jnp.concatenate([-jnp.ones((group_rows,), jnp.int32), doc_of], axis=0)

    def one_block(q_index):
        q_start = (q_index * block_rows).astype(jnp.int32)
        q_block = lax.dynamic_slice_in_dim(queries, q_start, block_rows, 0).astype(jnp.float32)
        q_block = q_block.reshape(block_rows, HEADS, qk_width)
        k_nope = lax.dynamic_slice_in_dim(keys_front, q_start, key_span, 0).astype(jnp.float32)
        k_nope = k_nope.reshape(key_span, HEADS, NOPE)
        k_rope = lax.dynamic_slice_in_dim(rope_front, q_start, key_span, 0).astype(jnp.float32)
        k_values = lax.dynamic_slice_in_dim(values_front, q_start, key_span, 0).astype(jnp.float32)
        k_values = k_values.reshape(key_span, HEADS, VDIM)
        q_docs = lax.dynamic_slice_in_dim(doc_of, q_start, block_rows, 0)
        k_docs = lax.dynamic_slice_in_dim(docs_front, q_start, key_span, 0)
        q_places = q_start + jnp.arange(block_rows, dtype=jnp.int32)
        k_places = q_start - group_rows + jnp.arange(key_span, dtype=jnp.int32)
        scores = jnp.einsum('ihd,jhd->hij', q_block[:, :, :NOPE], k_nope)
        scores = (scores + jnp.einsum('ihd,jd->hij', q_block[:, :, NOPE:], k_rope)) * score_scale
        allowed = (q_docs[:, None] == k_docs[None, :]) & (k_places[None, :] <= q_places[:, None])
        scores = jnp.where(allowed[None, :, :], scores, -jnp.inf)
        row_peak = lax.optimization_barrier(jnp.max(scores, axis=2, keepdims=True))
        expo = jnp.exp(scores - row_peak)
        row_sum = lax.optimization_barrier(jnp.sum(expo, axis=2))
        rounded = lax.optimization_barrier(expo.astype(jnp.bfloat16)).astype(jnp.float32)
        mixed = jnp.einsum('hij,jhd->ihd', rounded, k_values) / jnp.transpose(row_sum)[:, :, None]
        return mixed.reshape(block_rows, HEADS * VDIM).astype(jnp.bfloat16)
    attended = lax.map(one_block, jnp.arange(total_rows // block_rows, dtype=jnp.int32))
    return attended.reshape(total_rows, HEADS * VDIM)
```

```python
import functools
import math

import jax
import jax.numpy as jnp
from jax import lax
from jax.experimental import pallas as pl
from jax.experimental.pallas import tpu as pltpu
from jax.sharding import PartitionSpec as P

NOPE = 128
ROPE = 64
VDIM = 128
QK = NOPE + ROPE
LOG2E = 1.4426950408889634

MESH = pl.DeviceIdType.MESH


def kernel(
    sizes, queries, latent, rope_keys, key_weight, value_weight, lengths, out,
    lat_all, rope_all, w, qbuf, kaug, vbuf, bias, obuf,
    lat_sem, lat_send, w_own, w_recv, w_send, x_send, q_sem, q_send, o_sem, o_send,
):
    n_seq, n_head, look, wide, chunk_heads = sizes
    tok, rank = latent.shape
    half = n_seq // 2
    xs = n_head // 2
    slots = look + n_head
    span = (look + 1) * tok
    cw = chunk_heads * NOPE
    qw = chunk_heads * QK
    pieces = wide + xs
    q_all, o_all = (wide + 1) * qw, (wide + 1) * cw
    seq, head = lax.axis_index("seq"), lax.axis_index("head")
    core, x = head % 2, head // 2
    mate = head + 1 - 2 * core

    odd = seq % 2
    place = (seq // 2) * (1 - odd) + (n_seq - 1 - seq // 2) * odd

    def at_place(where):
        where = (where + n_seq) % n_seq
        fold = where // half
        return 2 * where * (1 - fold) + (2 * (n_seq - 1 - where) + 1) * fold

    after, before = at_place(place + 1), at_place(place - 1)

    shown = head - (n_head - look)
    gives = (shown >= 0) & (seq < n_seq - 1)
    takes = (shown >= 0) & (seq > 0)

    barrier = pltpu.get_barrier_semaphore()

    def greet(to_seq, to_head):
        pl.semaphore_signal(barrier, inc=1, device_id=(to_seq, to_head), device_id_type=MESH)

    greet(after, head)
    greet(before, head)
    for k in range(1, n_head):
        greet(seq, (head + k) % n_head)

    @pl.when(gives)
    def _():
        greet(seq + 1, head)

    @pl.when(takes)
    def _():
        greet(seq - 1, head)

    def owner(k, side):
        return ((x + k) % xs) * 2 + side

    def q_cols(who, c):
        return pl.ds(pl.multiple_of(who * q_all + c * qw, 128), qw)

    def o_cols(who, c):
        return pl.ds(pl.multiple_of(who * o_all + c * cw, 128), cw)

    def own_copies():
        mine = look + head
        pltpu.make_async_copy(latent, lat_all.at[mine], lat_sem.at[mine, 0]).start()
        pltpu.make_async_copy(rope_keys, rope_all.at[mine], lat_sem.at[mine, 1]).start()
        for c in range(wide + 1):
            for kv, source in enumerate((key_weight, value_weight)):
                pltpu.make_async_copy(
                    source.at[:, pl.ds(c * cw, cw)], w.at[c, seq, kv], w_own.at[c]
                ).start()
        for c in range(wide):
            pltpu.make_async_copy(
                queries.at[:, q_cols(head, c)], qbuf.at[c, head], q_sem.at[c]
            ).start()
        for k in range(xs):
            pltpu.make_async_copy(
                queries.at[:, q_cols(owner(k, core), wide)],
                qbuf.at[wide + k, core], q_sem.at[wide + k],
            ).start()

    own_copies()
    with jax.named_scope("barrier"):
        pl.semaphore_wait(
            barrier, n_head + 1 + gives.astype(jnp.int32) + takes.astype(jnp.int32)
        )

    def lat_copies(index, own, slot, to):
        return [
            pltpu.make_async_remote_copy(
                src_ref=given if own else held.at[slot], dst_ref=held.at[slot],
                send_sem=lat_send.at[index, part], recv_sem=lat_sem.at[slot, part],
                device_id=to, device_id_type=MESH,
            )
            for part, (given, held) in enumerate(((latent, lat_all), (rope_keys, rope_all)))
        ]

    def lat_wait(slot):
        for part, held in enumerate((lat_all, rope_all)):
            pltpu.make_async_copy(held.at[slot], held.at[slot], lat_sem.at[slot, part]).wait()

    def lat_out():
        sent = [lat_copies(k - 1, True, look + head, (seq, owner(k, core))) for k in range(1, xs)]
        return sent + [lat_copies(xs - 1, True, look + head, (seq, mate))]

    def back_out():
        return lat_copies(xs, True, shown, (seq + 1, head))

    def lat_on(k):
        return lat_copies(xs + k, False, look + owner(k, core), (seq, mate))

    def back_on(k):
        return lat_copies(2 * xs + k - 1, False, shown, (seq, owner(k, core)))

    def back_mate(i):
        return lat_copies(3 * xs - 1 + i, False, i, (seq, mate))

    def back_side(i):
        return core == (n_head - look + i) % 2

    def start(copies):
        for copy in copies:
            copy.start()

    def x_copies(k):
        return [
            pltpu.make_async_remote_copy(
                src_ref=source.at[:, pl.ds(wide * cw, cw)], dst_ref=w.at[wide + k, seq, kv],
                send_sem=x_send.at[k - 1], recv_sem=w_own.at[wide + k],
                device_id=(seq, owner(xs - k, core)), device_id_type=MESH,
            )
            for kv, source in enumerate((key_weight, value_weight))
        ]

    def own_weights(c):
        mine = w.at[c, seq]
        pltpu.make_async_copy(mine, mine, w_own.at[c]).wait()

    def ring_copies(c, t, way):
        origin = at_place(place - (t - 1)) if way == 0 else at_place(place + (t - 1))
        if t == half:
            pairs = [(w.at[c, origin, way], w.at[c, origin, way])]
        elif t == 1 and c <= wide:
            pairs = [
                (source.at[:, pl.ds(c * cw, cw)], w.at[c, origin, kv])
                for kv, source in enumerate((key_weight, value_weight))
            ]
        else:
            pairs = [(w.at[c, origin], w.at[c, origin])]
        return [
            pltpu.make_async_remote_copy(
                src_ref=src, dst_ref=dst, send_sem=w_send, recv_sem=w_recv.at[c, t - 1, way],
                device_id=(after if way == 0 else before, head), device_id_type=MESH,
            )
            for src, dst in pairs
        ]

    def ring_start(c):
        if c > wide:
            own_weights(c)
        for way in range(2):
            start(ring_copies(c, 1, way))

    def ring_take(c, t):
        for way in range(2):
            origin = at_place(place - t) if way == 0 else at_place(place + t)
            landed = w.at[c, origin, way] if t == half else w.at[c, origin]
            pltpu.make_async_copy(landed, landed, w_recv.at[c, t - 1, way]).wait()
            if t < half:
                start(ring_copies(c, t + 1, way))

    def q_copies(c):
        if c < wide:
            routes = [((head + k) % n_head,) * 2 + (head,) for k in range(1, n_head)]
        else:
            routes = [(mate, owner(c - wide, 1 - core), core)]
        return [
            pltpu.make_async_remote_copy(
                src_ref=queries.at[:, q_cols(who, min(c, wide))], dst_ref=qbuf.at[c, slot],
                send_sem=q_send.at[0 if c < wide else 1], recv_sem=q_sem.at[c],
                device_id=(seq, peer), device_id_type=MESH,
            )
            for peer, who, slot in routes
        ]

    def tile_at(c, j):
        if c >= wide:
            return 1 - core if j == 0 else core
        if j < n_head - 2:
            return (2 * x + 2 + j) % n_head
        return mate if j == n_head - 2 else head

    def o_copy(c, j):
        tile = tile_at(c, j)
        peer, who = (tile, head) if c < wide else (mate, owner(c - wide, core))
        return pltpu.make_async_remote_copy(
            src_ref=obuf.at[c, tile], dst_ref=out.at[:, o_cols(who, min(c, wide))],
            send_sem=o_send.at[0 if c < wide else 1], recv_sem=o_sem,
            device_id=(seq, peer), device_id_type=MESH,
        )

    start([copy for copies in lat_out() for copy in copies])

    @pl.when(gives)
    def _():
        start(back_out())

    ring_start(0)
    start(q_copies(0))
    ring_start(1)
    for c in range(wide, pieces):
        start(q_copies(c))

    docs = lengths.shape[0]
    first = seq * n_head * tok

    def mask_tile(j, carry):
        q_place = first + j * tok + lax.broadcasted_iota(jnp.int32, (tok, 1), 0)

        def document(d, state):
            begin, begun = state
            return begin + lengths[d], jnp.where(begin <= q_place, begin, begun)

        _, begun = lax.fori_loop(
            0, docs, document, (jnp.int32(0), jnp.zeros((tok, 1), jnp.int32)), unroll=True
        )
        k_place = first + (j - look) * tok + lax.broadcasted_iota(jnp.int32, (tok, span), 1)
        seen = (k_place >= begun) & (k_place <= q_place)
        bias[j] = jnp.where(seen, 0.0, -jnp.inf)
        return carry

    with jax.named_scope("mask"):
        lax.fori_loop(0, n_head, mask_tile, 0)

        @pl.when(seq == 0)
        def _():
            lat_all[:look] = jnp.zeros((look, tok, rank), jnp.bfloat16)
            rope_all[:look] = jnp.zeros((look, ROPE, tok), jnp.bfloat16)

        for h in range(chunk_heads):
            vbuf[:, (2 * h + 1) * VDIM:(2 * h + 2) * VDIM] = jnp.ones(
                (slots * tok, VDIM), jnp.bfloat16
            )

    def lat_relay():
        for k in range(1, xs):
            lat_wait(look + owner(k, core))
            start(lat_on(k))

    def back_relay():
        @pl.when(takes)
        def _():
            lat_wait(shown)
            for k in range(1, xs):
                start(back_on(k))

    def back_relay_mate():
        for i in range(look):
            @pl.when(back_side(i) & (seq > 0))
            def _():
                @pl.when(head != n_head - look + i)
                def _():
                    lat_wait(i)

                start(back_mate(i))

    def lat_done():
        lat_wait(look + head)
        for k in range(xs):
            lat_wait(look + owner(k, 1 - core))
        for i in range(look):
            @pl.when(jnp.logical_not(back_side(i)) & (seq > 0))
            def _():
                lat_wait(i)

    def rope_in():
        first_half = lax.broadcasted_iota(jnp.int32, (tok, 2 * ROPE), 1) < ROPE

        def fill(slot, carry):
            rope = rope_all[slot].astype(jnp.float32)
            twice = jnp.concatenate([rope, rope], axis=0).T
            at = pl.ds(pl.multiple_of(slot * tok, tok), tok)
            for h in range(chunk_heads):
                laid = jnp.where(first_half, twice, 0.0) if h % 2 == 0 else twice
                kaug[h, at, NOPE:] = laid.astype(jnp.bfloat16)
            return carry

        lax.fori_loop(0, slots, fill, 0)

    def project(c):
        if c <= wide:
            own_weights(c)
        first_slot, tiles = (0, slots) if c < wide else (2 * x, look + 2)
        parts = -(-tiles // 6)
        done = 0
        for part in range(parts):
            many = (tiles - done) // (parts - part)
            slot = first_slot + done
            done += many
            block = many * tok
            at = pl.ds(pl.multiple_of(slot * tok, tok), block)
            lat = lat_all[pl.ds(slot, many)].reshape(block, rank)
            low = lax.broadcasted_iota(jnp.int32, (block, NOPE), 1) < ROPE
            for pair in range(chunk_heads // 2):
                cols = slice(pair * 2 * NOPE, (pair + 1) * 2 * NOPE)
                k = jnp.dot(
                    lat, w[c, :, 0, :, cols].reshape(rank, 2 * NOPE),
                    preferred_element_type=jnp.float32,
                )
                kaug[2 * pair, at, :NOPE] = k[:, :NOPE].astype(jnp.bfloat16)
                turned = pltpu.roll(k[:, NOPE:], ROPE, axis=1)
                kaug[2 * pair + 1, at, :NOPE] = jnp.where(low, 0.0, turned).astype(jnp.bfloat16)
                rope_last = kaug[2 * pair + 1, at, NOPE:].astype(jnp.float32)
                kaug[2 * pair + 1, at, NOPE:] = jnp.where(low, turned, rope_last).astype(
                    jnp.bfloat16
                )
                v = jnp.dot(
                    lat, w[c, :, 1, :, cols].reshape(rank, 2 * VDIM),
                    preferred_element_type=jnp.float32,
                )
                for side in range(2):
                    begin = (2 * pair + side) * 2 * VDIM
                    vbuf[at, begin:begin + VDIM] = v[:, side * VDIM:(side + 1) * VDIM].astype(
                        jnp.bfloat16
                    )

    scale = LOG2E / math.sqrt(QK)

    def attend(c, j):
        tile = tile_at(c, j)
        place_of = tile if c < wide else 2 * x + tile
        at = pl.ds(pl.multiple_of(place_of * tok, tok), span)
        hide = bias[place_of]
        for h in range(chunk_heads):
            begin = (h // 2) * 2 * QK + (h % 2) * NOPE
            q = qbuf[c, tile, :, begin:begin + 2 * NOPE]
            s = lax.dot_general(
                q, kaug[h, at, :], (((1,), (1,)), ((), ())),
                preferred_element_type=jnp.float32,
            )
            s = s * scale + hide
            peak = jnp.max(s, axis=1, keepdims=True)
            expo = jnp.exp2(s - peak).astype(jnp.bfloat16)
            both = jnp.dot(
                expo, vbuf[at, h * 2 * VDIM:(h + 1) * 2 * VDIM],
                preferred_element_type=jnp.float32,
            )
            given = (both[:, :VDIM] / both[:, VDIM:]).astype(jnp.bfloat16)
            obuf[c, tile, :, h * VDIM:(h + 1) * VDIM] = given

    def q_in(c):
        landed = qbuf.at[c] if c < wide else qbuf.at[c, pl.ds(0, 2)]
        pltpu.make_async_copy(landed, landed, q_sem.at[c]).wait()

    def work_on(c):
        tiles = n_head if c < wide else 2

        def keys():
            with jax.named_scope(f"project{c}"):
                project(c)

        def tile(j):
            if j == 0:
                with jax.named_scope(f"q_in{c}"):
                    q_in(c)
            with jax.named_scope(f"attend{c}_{j}"):
                attend(c, j)
                if j < tiles - 1:
                    o_copy(c, j).start()
                else:
                    who = head if c < wide else owner(c - wide, core)
                    out[:, o_cols(who, min(c, wide))] = obuf[c, tile_at(c, j)]

        return [(0.8, keys)] + [(0.6, functools.partial(tile, j)) for j in range(tiles)]

    begins = {(0, half // 2): 2} | {(c - 3, half): c for c in range(3, pieces)}
    chores = {
        0: [lat_relay],
        1: [back_relay] + [lambda c=c: start(q_copies(c)) for c in range(1, min(2, wide))]
        + [lambda k=k: start(x_copies(k)) for k in range(1, xs)],
        2: [back_relay_mate],
        3: [lambda c=c: start(q_copies(c)) for c in range(2, wide)] + [lat_done, rope_in],
    }
    flight, waiting, number = [(0, 1), (1, 1)], [], 0
    while flight:
        c, t = flight.pop(0)
        with jax.named_scope(f"ring{c}_{t}"):
            ring_take(c, t)
        if t < half:
            flight.append((c, t + 1))
        if (c, t) in begins:
            ring_start(begins[c, t])
            flight.append((begins[c, t], 1))
        for chore in chores.get(number, []):
            with jax.named_scope(f"chore{number}"):
                chore()
        number += 1
        if t == half:
            waiting += work_on(c)
        room = 1.8
        while waiting and room > 0:
            cost, step = waiting.pop(0)
            step()
            room -= cost
    for _, step in waiting:
        step()

    with jax.named_scope("last"):
        landed = out.at[:, pl.ds(0, (wide * (n_head - 1) + xs) * cw)]
        pltpu.make_async_copy(landed, landed, o_sem).wait()

    def sent(ref, sem):
        pltpu.make_async_copy(ref, ref, sem).wait()

    with jax.named_scope("sends"):
        sent(obuf.at[pl.ds(0, wide), pl.ds(0, n_head - 1)], o_send.at[0])
        sent(obuf.at[pl.ds(wide, xs), pl.ds(0, 1)], o_send.at[1])
        sent(qbuf.at[pl.ds(0, wide), pl.ds(0, n_head - 1)], q_send.at[0])
        sent(qbuf.at[pl.ds(wide, xs), pl.ds(0, 1)], q_send.at[1])
        sent(w.at[:, pl.ds(0, n_seq - 1)], w_send)
        for k in range(1, xs):
            sent(w.at[wide + k, seq], x_send.at[k - 1])
        for copies in lat_out() + [lat_on(k) for k in range(1, xs)]:
            for copy in copies:
                copy.wait_send()

        @pl.when(gives)
        def _():
            for copy in back_out():
                copy.wait_send()

        @pl.when(takes)
        def _():
            for k in range(1, xs):
                for copy in back_on(k):
                    copy.wait_send()

        for i in range(look):
            @pl.when(back_side(i) & (seq > 0))
            def _():
                for copy in back_mate(i):
                    copy.wait_send()


def shards(queries, latent, rope_keys, key_weight, value_weight, doc_lengths):
    n_seq, n_head = lax.axis_size("seq"), lax.axis_size("head")
    tok, rank = latent.shape
    rows = key_weight.shape[0]
    local_heads = key_weight.shape[1] // NOPE
    docs = doc_lengths.shape[0]
    slot_rows = n_seq * n_head * tok // docs
    look = 2 * -(-slot_rows // tok) - 1
    chunk_heads = min(4, local_heads)
    wide = local_heads // chunk_heads - 1
    xs = n_head // 2
    pieces = wide + xs
    slots, span, half = look + n_head, (look + 1) * tok, n_seq // 2
    cw, qw = chunk_heads * NOPE, chunk_heads * QK
    anywhere = pl.BlockSpec(memory_space=pl.ANY)
    dma = pltpu.SemaphoreType.DMA
    bf16 = jnp.bfloat16
    return pl.pallas_call(
        functools.partial(kernel, (n_seq, n_head, look, wide, chunk_heads)),
        out_shape=pltpu.VMEM((tok, n_head * local_heads * VDIM), bf16),
        in_specs=[anywhere] * 5 + [pl.BlockSpec(memory_space=pltpu.SMEM)],
        out_specs=pl.BlockSpec(memory_space=pltpu.VMEM),
        scratch_shapes=[
            pltpu.VMEM((slots, tok, rank), bf16),
            pltpu.VMEM((slots, ROPE, tok), bf16),
            pltpu.VMEM((pieces, n_seq, 2, rows, cw), bf16),
            pltpu.VMEM((pieces, n_head, tok, qw), bf16),
            pltpu.VMEM((chunk_heads, slots * tok, 2 * NOPE), bf16),
            pltpu.VMEM((slots * tok, 2 * cw), bf16),
            pltpu.VMEM((n_head, tok, span), jnp.float32),
            pltpu.VMEM((pieces, n_head, tok, cw), bf16),
            dma((slots, 2)),
            dma((3 * xs - 1 + look, 2)),
            dma((pieces,)),
            dma((pieces, half, 2)),
            dma,
            dma((xs - 1,)),
            dma((pieces,)),
            dma((2,)),
            dma,
            dma((2,)),
        ],
        compiler_params=pltpu.CompilerParams(collective_id=0, has_side_effects=True),
    )(queries, latent, rope_keys.T, key_weight, value_weight, doc_lengths)


def solution(mesh):
    placed = (
        P(("seq", "head"), None),
        P(("seq", "head"), None),
        P(("seq", "head"), None),
        P("seq", "head"),
        P("seq", "head"),
        P(),
    )
    return jax.shard_map(
        shards, mesh=mesh, in_specs=placed, out_specs=P(("seq", "head"), None), check_vma=False
    )
```

```python
import functools
import math

import jax
import jax.numpy as jnp
from jax import lax
from jax.experimental import pallas as pl
from jax.experimental.pallas import tpu as pltpu
from jax.sharding import PartitionSpec as P

NOPE = 128
ROPE = 64
VDIM = 128
QK = NOPE + ROPE
LOG2E = 1.4426950408889634

MESH = pl.DeviceIdType.MESH


def ring_order(pieces, wide, steps_of):
    if (pieces, wide, steps_of(0)) == (5, 3, 4):
        steps = (1, 11, 2, 12, 3, 31, 21, 13, 4, 22, 14, 32, 41, 23, 42, 24, 33, 43, 34)
        return [divmod(step, 10) for step in steps], {4: (2, 2)}
    first = [0, wide] + list(range(1, wide))
    flight, later, order = [(c, 1) for c in first[:2]], first[2:] + list(range(wide + 1, pieces)), []
    while flight:
        c, t = flight.pop(0)
        order.append((c, t))
        if t < steps_of(c):
            flight.append((c, t + 1))
        if t >= steps_of(c) // 2 and later and len(flight) < 3:
            flight.append((later.pop(0), 1))
    holds = {}
    for c in range(wide + 1, pieces):
        at = order.index((c, 1))
        holds[c] = order[max(at - 2, order.index((wide, 1)))]
    return order, holds


def kernel(
    sizes, queries, latent, rope_keys, key_weight, value_weight, lengths_in, out,
    lat_all, rope_all, w, qbuf, kaug, vbuf, bias, obuf, lengths,
    len_sem, lat_sem, lat_send, w_own, w_recv, w_send, x_send, x_recv, q_sem, q_send, o_sem, o_send,
):
    n_seq, n_head, look, wide, chunk_heads = sizes
    tok, rank = latent.shape
    half = n_seq // 2
    xs = n_head // 2
    slots = look + n_head
    span = (look + 1) * tok
    cw = chunk_heads * NOPE
    qw = chunk_heads * QK
    pieces = wide + xs
    q_all, o_all = (wide + 1) * qw, (wide + 1) * cw
    seq, head = lax.axis_index("seq"), lax.axis_index("head")
    core, x = head % 2, head // 2
    mate = head + 1 - 2 * core

    odd = seq % 2
    place = (seq // 2) * (1 - odd) + (n_seq - 1 - seq // 2) * odd

    def at_place(where):
        where = (where + n_seq) % n_seq
        fold = where // half
        return 2 * where * (1 - fold) + (2 * (n_seq - 1 - where) + 1) * fold

    after, before = at_place(place + 1), at_place(place - 1)

    shown = head - (n_head - look)
    gives = (shown >= 0) & (seq < n_seq - 1)
    takes = (shown >= 0) & (seq > 0)

    barrier = pltpu.get_barrier_semaphore()

    def greet(to_seq, to_head):
        pl.semaphore_signal(barrier, inc=1, device_id=(to_seq, to_head), device_id_type=MESH)

    greet(after, head)
    greet(before, head)
    for k in range(1, n_head):
        greet(seq, (head + k) % n_head)

    @pl.when(gives)
    def _():
        greet(seq + 1, head)

    @pl.when(takes)
    def _():
        greet(seq - 1, head)

    def owner(k, side):
        return ((x + k) % xs) * 2 + side

    def q_cols(who, c):
        return pl.ds(pl.multiple_of(who * q_all + c * qw, 128), qw)

    def o_cols(who, c):
        return pl.ds(pl.multiple_of(who * o_all + c * cw, 128), cw)

    def own_copies():
        for c in range(wide + 1):
            for kv, source in enumerate((key_weight, value_weight)):
                pltpu.make_async_copy(
                    source.at[:, pl.ds(c * cw, cw)], w.at[c, seq, kv], w_own.at[c]
                ).start()
        mine = look + head
        pltpu.make_async_copy(latent, lat_all.at[mine], lat_sem.at[mine, 0]).start()
        pltpu.make_async_copy(rope_keys, rope_all.at[mine], lat_sem.at[mine, 1]).start()
        for c in range(wide):
            pltpu.make_async_copy(
                queries.at[:, q_cols(head, c)], qbuf.at[c, head], q_sem.at[c]
            ).start()
        for k in range(xs):
            pltpu.make_async_copy(
                queries.at[:, q_cols(owner(k, core), wide)],
                qbuf.at[wide + k, core], q_sem.at[wide + k],
            ).start()

    own_copies()
    pltpu.make_async_copy(lengths_in, lengths, len_sem).start()
    with jax.named_scope("barrier"):
        pl.semaphore_wait(
            barrier, n_head + 1 + gives.astype(jnp.int32) + takes.astype(jnp.int32)
        )

    def lat_copies(index, slot, to, landing):
        return [
            pltpu.make_async_remote_copy(
                src_ref=held.at[slot], dst_ref=held.at[landing],
                send_sem=lat_send.at[index, part], recv_sem=lat_sem.at[landing, part],
                device_id=to, device_id_type=MESH,
            )
            for part, held in enumerate((lat_all, rope_all))
        ]

    def lat_wait(slot):
        for part, held in enumerate((lat_all, rope_all)):
            pltpu.make_async_copy(held.at[slot], held.at[slot], lat_sem.at[slot, part]).wait()

    mine = look + head

    def lat_out():
        sent = [lat_copies(k - 1, mine, (seq, owner(k, core)), mine) for k in range(1, xs)]
        return sent + [lat_copies(xs - 1, mine, (seq, mate), mine)]

    def back_out():
        return lat_copies(xs, mine, (seq + 1, head), shown)

    def lat_on(k):
        slot = look + owner(k, core)
        return lat_copies(xs + k, slot, (seq, mate), slot)

    def back_on(k):
        return lat_copies(2 * xs + k - 1, shown, (seq, owner(k, core)), shown)

    def back_mate(i):
        return lat_copies(3 * xs - 1 + i, i, (seq, mate), i)

    def back_side(i):
        return core == (n_head - look + i) % 2

    def start(copies):
        for copy in copies:
            copy.start()

    def x_copy(k, near):
        rows_of = seq if near == 0 else before
        return pltpu.make_async_remote_copy(
            src_ref=w.at[wide, rows_of], dst_ref=w.at[wide + k, rows_of],
            send_sem=x_send.at[k - 1, near], recv_sem=x_recv.at[k - 1, near],
            device_id=(seq, owner(xs - k, core)), device_id_type=MESH,
        )

    def landed_rows(c):
        if c <= wide:
            pltpu.make_async_copy(w.at[c, seq], w.at[c, seq], w_own.at[c]).wait()
        else:
            for near, rows_of in enumerate((seq, before)):
                here = w.at[c, rows_of]
                pltpu.make_async_copy(here, here, x_recv.at[c - wide - 1, near]).wait()

    def steps_of(c):
        return half if c <= wide else half - 1

    def origin_at(c, t, way):
        return at_place(place - t - (c > wide)) if way == 0 else at_place(place + t)

    def ring_copy(c, t, way):
        origin = origin_at(c, t - 1, way)
        block = w.at[c, origin, way] if t == half else w.at[c, origin]
        return pltpu.make_async_remote_copy(
            src_ref=block, dst_ref=block, send_sem=w_send.at[0 if c <= wide else 1],
            recv_sem=w_recv.at[c, t - 1],
            device_id=(after if way == 0 else before, head), device_id_type=MESH,
        )

    def ring_send(c, t):
        if t == 1 and c > wide:
            landed_rows(c)
        for way in range(2):
            ring_copy(c, t, way).start()

    def ring_take(c, t):
        landed = w.at[c, 0] if t == half else w.at[c, pl.ds(0, 2)]
        pltpu.make_async_copy(landed, landed, w_recv.at[c, t - 1]).wait()

    def q_copies(c):
        if c < wide:
            routes = [((head + k) % n_head,) * 2 + (head,) for k in range(1, n_head)]
        else:
            routes = [(mate, owner(c - wide, 1 - core), core)]
        return [
            pltpu.make_async_remote_copy(
                src_ref=queries.at[:, q_cols(who, min(c, wide))], dst_ref=qbuf.at[c, slot],
                send_sem=q_send.at[0 if c < wide else 1], recv_sem=q_sem.at[c],
                device_id=(seq, peer), device_id_type=MESH,
            )
            for peer, who, slot in routes
        ]

    def tile_at(c, j):
        if c >= wide:
            return 1 - core if j == 0 else core
        if j < n_head - 2:
            return (2 * x + 2 + j) % n_head
        return mate if j == n_head - 2 else head

    def o_copy(c, j):
        tile = tile_at(c, j)
        peer, who = (tile, head) if c < wide else (mate, owner(c - wide, core))
        return pltpu.make_async_remote_copy(
            src_ref=obuf.at[c, tile], dst_ref=out.at[:, o_cols(who, min(c, wide))],
            send_sem=o_send.at[0 if c < wide else 1], recv_sem=o_sem,
            device_id=(seq, peer), device_id_type=MESH,
        )

    order, holds = ring_order(pieces, wide, steps_of)
    for c in range(wide + 1):
        landed_rows(c)
        if c == 0:
            ring_send(*order[0])
    ring_send(*order[1])
    lat_wait(mine)
    start([copy for copies in lat_out() for copy in copies])
    start(q_copies(0))

    @pl.when(gives)
    def _():
        start(back_out())

    for c in range(wide, pieces):
        start(q_copies(c))

    docs = lengths.shape[0]
    first = seq * n_head * tok

    def mask_tile(j, carry):
        q_place = first + j * tok + lax.broadcasted_iota(jnp.int32, (tok, 1), 0)

        def document(d, state):
            begin, begun = state
            return begin + lengths[d], jnp.where(begin <= q_place, begin, begun)

        _, begun = lax.fori_loop(
            0, docs, document, (jnp.int32(0), jnp.zeros((tok, 1), jnp.int32)), unroll=True
        )
        k_place = first + (j - look) * tok + lax.broadcasted_iota(jnp.int32, (tok, span), 1)
        seen = (k_place >= begun) & (k_place <= q_place)
        bias[j] = jnp.where(seen, 0.0, -jnp.inf)
        return carry

    with jax.named_scope("mask"):
        pltpu.make_async_copy(lengths_in, lengths, len_sem).wait()
        lax.fori_loop(0, n_head, mask_tile, 0)

        @pl.when(seq == 0)
        def _():
            lat_all[:look] = jnp.zeros((look, tok, rank), jnp.bfloat16)
            rope_all[:look] = jnp.zeros((look, ROPE, tok), jnp.bfloat16)

        for h in range(chunk_heads):
            vbuf[:, (2 * h + 1) * VDIM:(2 * h + 2) * VDIM] = jnp.ones(
                (slots * tok, VDIM), jnp.bfloat16
            )

    def lat_relay():
        for k in range(1, xs):
            lat_wait(look + owner(k, core))
            start(lat_on(k))

    def back_relay():
        @pl.when(takes)
        def _():
            lat_wait(shown)
            for k in range(1, xs):
                start(back_on(k))

    def back_relay_mate():
        for i in range(look):
            @pl.when(back_side(i) & (seq > 0))
            def _():
                @pl.when(head != n_head - look + i)
                def _():
                    lat_wait(i)

                start(back_mate(i))

    def lat_done():
        for k in range(xs):
            lat_wait(look + owner(k, 1 - core))
        for i in range(look):
            @pl.when(jnp.logical_not(back_side(i)) & (seq > 0))
            def _():
                lat_wait(i)

    def rope_in():
        first_half = lax.broadcasted_iota(jnp.int32, (tok, 2 * ROPE), 1) < ROPE

        def fill(slot, carry):
            rope = rope_all[slot].astype(jnp.float32)
            twice = jnp.concatenate([rope, rope], axis=0).T
            at = pl.ds(pl.multiple_of(slot * tok, tok), tok)
            for h in range(chunk_heads):
                laid = jnp.where(first_half, twice, 0.0) if h % 2 == 0 else twice
                kaug[h, at, NOPE:] = laid.astype(jnp.bfloat16)
            return carry

        lax.fori_loop(0, slots, fill, 0)

    def project(c):
        first_slot, tiles = (0, slots) if c < wide else (2 * x, look + 2)
        parts = -(-tiles // 6)
        done = 0
        for part in range(parts):
            many = (tiles - done) // (parts - part)
            slot = first_slot + done
            done += many
            block = many * tok
            at = pl.ds(pl.multiple_of(slot * tok, tok), block)
            lat = lat_all[pl.ds(slot, many)].reshape(block, rank)
            low = lax.broadcasted_iota(jnp.int32, (block, NOPE), 1) < ROPE
            for pair in range(chunk_heads // 2):
                cols = slice(pair * 2 * NOPE, (pair + 1) * 2 * NOPE)
                k = jnp.dot(
                    lat, w[c, :, 0, :, cols].reshape(rank, 2 * NOPE),
                    preferred_element_type=jnp.float32,
                )
                kaug[2 * pair, at, :NOPE] = k[:, :NOPE].astype(jnp.bfloat16)
                turned = pltpu.roll(k[:, NOPE:], ROPE, axis=1)
                kaug[2 * pair + 1, at, :NOPE] = jnp.where(low, 0.0, turned).astype(jnp.bfloat16)
                rope_last = kaug[2 * pair + 1, at, NOPE:].astype(jnp.float32)
                kaug[2 * pair + 1, at, NOPE:] = jnp.where(low, turned, rope_last).astype(
                    jnp.bfloat16
                )
                v = jnp.dot(
                    lat, w[c, :, 1, :, cols].reshape(rank, 2 * VDIM),
                    preferred_element_type=jnp.float32,
                )
                for side in range(2):
                    begin = (2 * pair + side) * 2 * VDIM
                    vbuf[at, begin:begin + VDIM] = v[:, side * VDIM:(side + 1) * VDIM].astype(
                        jnp.bfloat16
                    )

    scale = LOG2E / math.sqrt(QK)

    def attend(c, tiles, then):
        def places(tile):
            place_of = tile if c < wide else 2 * x + tile
            return place_of, pl.ds(pl.multiple_of(place_of * tok, tok), span)

        def scores(tile, h):
            begin = (h // 2) * 2 * QK + (h % 2) * NOPE
            return lax.dot_general(
                qbuf[c, tile, :, begin:begin + 2 * NOPE], kaug[h, places(tile)[1], :],
                (((1,), (1,)), ((), ())), preferred_element_type=jnp.float32,
            )

        def weights(tile, s):
            s = s * scale + bias[places(tile)[0]]
            peak = jnp.max(s, axis=1, keepdims=True)
            return jnp.exp2(s - peak).astype(jnp.bfloat16)

        def mix(tile, h, expo):
            both = jnp.dot(
                expo, vbuf[places(tile)[1], h * 2 * VDIM:(h + 1) * 2 * VDIM],
                preferred_element_type=jnp.float32,
            )
            given = (both[:, :VDIM] / both[:, VDIM:]).astype(jnp.bfloat16)
            obuf[c, tile, :, h * VDIM:(h + 1) * VDIM] = given

        items = [(tile, h) for tile in tiles for h in range(chunk_heads)]
        held = [scores(tile, h) for tile, h in items]
        expo = {}
        for i, (tile, h) in enumerate(items):
            expo[i] = weights(tile, held[i])
            if i > 0:
                mix(*items[i - 1], expo.pop(i - 1))
            if i == chunk_heads and c >= wide:
                then[0]()
        mix(*items[-1], expo.pop(len(items) - 1))
        if c < wide:
            then[0]()
        then[1]()

    def q_in(c):
        landed = qbuf.at[c] if c < wide else qbuf.at[c, pl.ds(0, 2)]
        pltpu.make_async_copy(landed, landed, q_sem.at[c]).wait()

    def work_on(c):
        tiles = n_head if c < wide else 2

        def keys():
            with jax.named_scope(f"q_in{c}"):
                q_in(c)
            with jax.named_scope(f"project{c}"):
                project(c)

        def pair(j):
            def keep():
                who = head if c < wide else owner(c - wide, core)
                out[:, o_cols(who, min(c, wide))] = obuf[c, tile_at(c, j + 1)]

            first_sent = o_copy(c, j).start
            second_sent = o_copy(c, j + 1).start if j + 2 < tiles else keep
            with jax.named_scope(f"attend{c}_{j}"):
                attend(c, [tile_at(c, j), tile_at(c, j + 1)], (first_sent, second_sent))

        return [(0.8, keys)] + [(0.8, functools.partial(pair, j)) for j in range(0, tiles, 2)]

    chores = {
        (0, 1): [lat_relay],
        (1, 1): [back_relay] + [lambda c=c: start(q_copies(c)) for c in range(1, min(2, wide))]
        + [lambda k=k: x_copy(k, 0).start() for k in range(1, xs)],
        (0, 2): [back_relay_mate],
        (1, 2): [lat_done, rope_in],
    }
    chores.setdefault((wide, 1), []).extend(
        [lambda k=k: x_copy(k, 1).start() for k in range(1, xs)]
        + [lambda c=c: start(q_copies(c)) for c in range(2, wide)]
    )
    unsent, waiting, taken = order[2:], [], set()
    for c, t in order:
        with jax.named_scope(f"ring{c}_{t}"):
            ring_take(c, t)
        taken.add((c, t))
        while unsent:
            ahead, step = unsent[0]
            need = (ahead, step - 1) if step > 1 else holds.get(ahead)
            if need is not None and need not in taken:
                break
            ring_send(*unsent.pop(0))
        for chore in chores.get((c, t), []):
            with jax.named_scope("chore"):
                chore()
        if t == steps_of(c):
            waiting += work_on(c)
        room = 1.8
        while waiting and room > 0:
            cost, step = waiting.pop(0)
            step()
            room -= cost
    for _, step in waiting:
        step()

    with jax.named_scope("last"):
        landed = out.at[:, pl.ds(0, (wide * (n_head - 1) + xs) * cw)]
        pltpu.make_async_copy(landed, landed, o_sem).wait()

    def sent(ref, sem):
        pltpu.make_async_copy(ref, ref, sem).wait()

    with jax.named_scope("sends"):
        sent(obuf.at[pl.ds(0, wide), pl.ds(0, n_head - 1)], o_send.at[0])
        sent(obuf.at[pl.ds(wide, xs), pl.ds(0, 1)], o_send.at[1])
        sent(qbuf.at[pl.ds(0, wide), pl.ds(0, n_head - 1)], q_send.at[0])
        sent(qbuf.at[pl.ds(wide, xs), pl.ds(0, 1)], q_send.at[1])
        sent(w.at[pl.ds(0, wide + 1), pl.ds(0, n_seq - 1)], w_send.at[0])
        sent(w.at[pl.ds(wide + 1, xs - 1), pl.ds(0, n_seq - 2)], w_send.at[1])
        for k in range(1, xs):
            for near in range(2):
                x_copy(k, near).wait_send()
        for copies in lat_out() + [lat_on(k) for k in range(1, xs)]:
            for copy in copies:
                copy.wait_send()

        @pl.when(gives)
        def _():
            for copy in back_out():
                copy.wait_send()

        @pl.when(takes)
        def _():
            for k in range(1, xs):
                for copy in back_on(k):
                    copy.wait_send()

        for i in range(look):
            @pl.when(back_side(i) & (seq > 0))
            def _():
                for copy in back_mate(i):
                    copy.wait_send()


def shards(queries, latent, rope_keys, key_weight, value_weight, doc_lengths):
    n_seq, n_head = lax.axis_size("seq"), lax.axis_size("head")
    tok, rank = latent.shape
    rows = key_weight.shape[0]
    local_heads = key_weight.shape[1] // NOPE
    docs = doc_lengths.shape[0]
    slot_rows = n_seq * n_head * tok // docs
    look = 2 * -(-slot_rows // tok) - 1
    chunk_heads = min(4, local_heads)
    wide = local_heads // chunk_heads - 1
    xs = n_head // 2
    pieces = wide + xs
    slots, span, half = look + n_head, (look + 1) * tok, n_seq // 2
    cw, qw = chunk_heads * NOPE, chunk_heads * QK
    anywhere = pl.BlockSpec(memory_space=pl.ANY)
    dma = pltpu.SemaphoreType.DMA
    bf16 = jnp.bfloat16
    return pl.pallas_call(
        functools.partial(kernel, (n_seq, n_head, look, wide, chunk_heads)),
        out_shape=pltpu.VMEM((tok, n_head * local_heads * VDIM), bf16),
        in_specs=[anywhere] * 6,
        out_specs=pl.BlockSpec(memory_space=pltpu.VMEM),
        scratch_shapes=[
            pltpu.VMEM((slots, tok, rank), bf16),
            pltpu.VMEM((slots, ROPE, tok), bf16),
            pltpu.VMEM((pieces, n_seq, 2, rows, cw), bf16),
            pltpu.VMEM((pieces, n_head, tok, qw), bf16),
            pltpu.VMEM((chunk_heads, slots * tok, 2 * NOPE), bf16),
            pltpu.VMEM((slots * tok, 2 * cw), bf16),
            pltpu.VMEM((n_head, tok, span), jnp.float32),
            pltpu.VMEM((pieces, n_head, tok, cw), bf16),
            pltpu.SMEM((docs,), jnp.int32),
            dma,
            dma((slots, 2)),
            dma((3 * xs - 1 + look, 2)),
            dma((wide + 1,)),
            dma((pieces, half)),
            dma((2,)),
            dma((xs - 1, 2)),
            dma((xs - 1, 2)),
            dma((pieces,)),
            dma((2,)),
            dma,
            dma((2,)),
        ],
        compiler_params=pltpu.CompilerParams(collective_id=0, has_side_effects=True),
    )(queries, latent, rope_keys.T, key_weight, value_weight, doc_lengths)


def solution(mesh):
    placed = (
        P(("seq", "head"), None),
        P(("seq", "head"), None),
        P(("seq", "head"), None),
        P("seq", "head"),
        P("seq", "head"),
        P(),
    )
    return jax.shard_map(
        shards, mesh=mesh, in_specs=placed, out_specs=P(("seq", "head"), None), check_vma=False
    )
```

```python
import functools
import math

import jax
import jax.numpy as jnp
from jax import lax
from jax.experimental import pallas as pl
from jax.experimental.pallas import tpu as pltpu
from jax.sharding import PartitionSpec as P

NOPE = 128
ROPE = 64
VDIM = 128
QK = NOPE + ROPE
LOG2E = 1.4426950408889634

MESH = pl.DeviceIdType.MESH


def ring_order(pieces, wide, steps_of):
    if (pieces, wide, steps_of(0)) == (5, 3, 4):
        steps = (1, 11, 2, 12, 3, 31, 21, 13, 4, 22, 14, 32, 41, 23, 42, 24, 33, 43, 34)
        return [divmod(step, 10) for step in steps], {4: (2, 2)}
    first = [0, wide] + list(range(1, wide))
    flight, later, order = [(c, 1) for c in first[:2]], first[2:] + list(range(wide + 1, pieces)), []
    while flight:
        c, t = flight.pop(0)
        order.append((c, t))
        if t < steps_of(c):
            flight.append((c, t + 1))
        if t >= steps_of(c) // 2 and later and len(flight) < 3:
            flight.append((later.pop(0), 1))
    holds = {}
    for c in range(wide + 1, pieces):
        at = order.index((c, 1))
        holds[c] = order[max(at - 2, order.index((wide, 1)))]
    return order, holds


def kernel(
    sizes, queries, latent, rope_keys, key_weight, value_weight, lengths_in, out,
    lat_all, rope_all, w, qbuf, kaug, vbuf, bias, obuf, lengths,
    len_sem, lat_sem, lat_send, w_own, w_recv, w_send, x_send, x_recv, q_sem, q_send, o_sem, o_send,
):
    n_seq, n_head, look, wide, chunk_heads = sizes
    tok, rank = latent.shape
    half = n_seq // 2
    xs = n_head // 2
    slots = look + n_head
    span = (look + 1) * tok
    cw = chunk_heads * NOPE
    qw = chunk_heads * QK
    pieces = wide + xs
    q_all, o_all = (wide + 1) * qw, (wide + 1) * cw
    seq, head = lax.axis_index("seq"), lax.axis_index("head")
    core, x = head % 2, head // 2
    mate = head + 1 - 2 * core

    odd = seq % 2
    place = (seq // 2) * (1 - odd) + (n_seq - 1 - seq // 2) * odd

    def at_place(where):
        where = (where + n_seq) % n_seq
        fold = where // half
        return 2 * where * (1 - fold) + (2 * (n_seq - 1 - where) + 1) * fold

    after, before = at_place(place + 1), at_place(place - 1)

    shown = head - (n_head - look)
    gives = (shown >= 0) & (seq < n_seq - 1)
    takes = (shown >= 0) & (seq > 0)

    barrier = pltpu.get_barrier_semaphore()

    def greet(to_seq, to_head):
        pl.semaphore_signal(barrier, inc=1, device_id=(to_seq, to_head), device_id_type=MESH)

    greet(after, head)
    greet(before, head)
    for k in range(1, n_head):
        greet(seq, (head + k) % n_head)

    @pl.when(gives)
    def _():
        greet(seq + 1, head)

    @pl.when(takes)
    def _():
        greet(seq - 1, head)

    def owner(k, side):
        return ((x + k) % xs) * 2 + side

    def q_cols(who, c):
        return pl.ds(pl.multiple_of(who * q_all + c * qw, 128), qw)

    def own_copies():
        for c in range(wide + 1):
            for kv, source in enumerate((key_weight, value_weight)):
                pltpu.make_async_copy(
                    source.at[:, pl.ds(c * cw, cw)], w.at[c, seq, kv], w_own
                ).start()
        mine = look + head
        pltpu.make_async_copy(latent, lat_all.at[mine], lat_sem.at[mine, 0]).start()
        pltpu.make_async_copy(rope_keys, rope_all.at[mine], lat_sem.at[mine, 1]).start()
        for c in range(wide):
            pltpu.make_async_copy(
                queries.at[:, q_cols(head, c)], qbuf.at[c, head], q_sem.at[c]
            ).start()
        for k in range(xs):
            pltpu.make_async_copy(
                queries.at[:, q_cols(owner(k, core), wide)],
                qbuf.at[wide + k, core], q_sem.at[wide + k],
            ).start()

    own_copies()
    pltpu.make_async_copy(lengths_in, lengths, len_sem).start()
    with jax.named_scope("barrier"):
        pl.semaphore_wait(
            barrier, n_head + 1 + gives.astype(jnp.int32) + takes.astype(jnp.int32)
        )

    def lat_copies(index, slot, to, landing):
        return [
            pltpu.make_async_remote_copy(
                src_ref=held.at[slot], dst_ref=held.at[landing],
                send_sem=lat_send.at[index, part], recv_sem=lat_sem.at[landing, part],
                device_id=to, device_id_type=MESH,
            )
            for part, held in enumerate((lat_all, rope_all))
        ]

    def lat_wait(slot):
        for part, held in enumerate((lat_all, rope_all)):
            pltpu.make_async_copy(held.at[slot], held.at[slot], lat_sem.at[slot, part]).wait()

    mine = look + head

    def lat_out():
        sent = [lat_copies(k - 1, mine, (seq, owner(k, core)), mine) for k in range(1, xs)]
        return sent + [lat_copies(xs - 1, mine, (seq, mate), mine)]

    def back_out():
        return lat_copies(xs, mine, (seq + 1, head), shown)

    def lat_on(k):
        slot = look + owner(k, core)
        return lat_copies(xs + k, slot, (seq, mate), slot)

    def back_on(k):
        return lat_copies(2 * xs + k - 1, shown, (seq, owner(k, core)), shown)

    def back_mate(i):
        return lat_copies(3 * xs - 1 + i, i, (seq, mate), i)

    def back_side(i):
        return core == (n_head - look + i) % 2

    def start(copies):
        for copy in copies:
            copy.start()

    def x_copy(k, near):
        rows_of = seq if near == 0 else before
        return pltpu.make_async_remote_copy(
            src_ref=w.at[wide, rows_of], dst_ref=w.at[wide + k, rows_of],
            send_sem=x_send.at[k - 1], recv_sem=x_recv.at[k - 1],
            device_id=(seq, owner(xs - k, core)), device_id_type=MESH,
        )

    def arrive(ref, sem):
        pltpu.make_async_copy(ref, ref, sem).wait()

    def steps_of(c):
        return half if c <= wide else half - 1

    def origin_at(c, t, way):
        return at_place(place - t - (c > wide)) if way == 0 else at_place(place + t)

    pairs = chunk_heads // 2

    def ring_copy(c, t, way):
        origin = origin_at(c, t - 1, way)
        block = w.at[c, origin, way] if t == half else w.at[c, origin]
        return pltpu.make_async_remote_copy(
            src_ref=block, dst_ref=block, send_sem=w_send.at[0 if c <= wide else 1],
            recv_sem=w_recv.at[c, t - 1],
            device_id=(after if way == 0 else before, head), device_id_type=MESH,
        )

    def ring_send(c, t):
        if t == 1 and c > wide:
            arrive(w.at[c, pl.ds(0, 2)], x_recv.at[c - wide - 1])
        for way in range(2):
            ring_copy(c, t, way).start()

    def ring_take(c, t):
        arrive(w.at[c, 0] if t == half else w.at[c, pl.ds(0, 2)], w_recv.at[c, t - 1])

    pairs = chunk_heads // 2

    def q_copies(c):
        if c < wide:
            routes = [((head + k) % n_head,) * 2 + (head,) for k in range(1, n_head)]
        else:
            routes = [(mate, owner(c - wide, 1 - core), core)]
        return [
            pltpu.make_async_remote_copy(
                src_ref=queries.at[:, q_cols(who, min(c, wide))], dst_ref=qbuf.at[c, slot],
                send_sem=q_send.at[0 if c < wide else 1], recv_sem=q_sem.at[c],
                device_id=(seq, peer), device_id_type=MESH,
            )
            for peer, who, slot in routes
        ]

    def tile_at(c, j):
        if c >= wide:
            return 1 - core if j == 0 else core
        if j < n_head - 2:
            return (2 * x + 2 + j) % n_head
        return mate if j == n_head - 2 else head

    def o_cols(who, c):
        return pl.ds(pl.multiple_of(who * o_all + min(c, wide) * cw, 128), cw)

    def o_copy(c, j):
        tile = tile_at(c, j)
        peer, who = (tile, head) if c < wide else (mate, owner(c - wide, core))
        return pltpu.make_async_remote_copy(
            src_ref=obuf.at[c, tile], dst_ref=out.at[:, o_cols(who, c)],
            send_sem=o_send.at[0 if c < wide else 1], recv_sem=o_sem,
            device_id=(seq, peer), device_id_type=MESH,
        )

    order, holds = ring_order(pieces, wide, steps_of)
    arrive(w.at[pl.ds(0, wide + 1), 0], w_own)
    ring_send(*order[0])
    ring_send(*order[1])
    lat_wait(mine)
    start([copy for copies in lat_out() for copy in copies])
    start(q_copies(0))

    @pl.when(gives)
    def _():
        start(back_out())

    for c in range(wide, pieces):
        start(q_copies(c))

    docs = lengths.shape[0]
    first = seq * n_head * tok

    def mask_tile(j, carry):
        q_place = first + j * tok + lax.broadcasted_iota(jnp.int32, (tok, 1), 0)

        def document(d, state):
            begin, begun = state
            return begin + lengths[d], jnp.where(begin <= q_place, begin, begun)

        _, begun = lax.fori_loop(
            0, docs, document, (jnp.int32(0), jnp.zeros((tok, 1), jnp.int32)), unroll=True
        )
        k_place = first + (j - look) * tok + lax.broadcasted_iota(jnp.int32, (tok, span), 1)
        seen = (k_place >= begun) & (k_place <= q_place)
        bias[j] = jnp.where(seen, 0.0, -jnp.inf)
        return carry

    with jax.named_scope("mask"):
        pltpu.make_async_copy(lengths_in, lengths, len_sem).wait()
        lax.fori_loop(0, n_head, mask_tile, 0)

        @pl.when(seq == 0)
        def _():
            lat_all[:look] = jnp.zeros((look, tok, rank), jnp.bfloat16)
            rope_all[:look] = jnp.zeros((look, ROPE, tok), jnp.bfloat16)

        for h in range(chunk_heads):
            vbuf[:, (2 * h + 1) * VDIM:(2 * h + 2) * VDIM] = jnp.ones(
                (slots * tok, VDIM), jnp.bfloat16
            )

    def lat_relay():
        for k in range(1, xs):
            lat_wait(look + owner(k, core))
            start(lat_on(k))

    def back_relay():
        @pl.when(takes)
        def _():
            lat_wait(shown)
            for k in range(1, xs):
                start(back_on(k))

    def back_relay_mate():
        for i in range(look):
            @pl.when(back_side(i) & (seq > 0))
            def _():
                @pl.when(head != n_head - look + i)
                def _():
                    lat_wait(i)

                start(back_mate(i))

    def lat_done():
        for k in range(xs):
            lat_wait(look + owner(k, 1 - core))
        for i in range(look):
            @pl.when(jnp.logical_not(back_side(i)) & (seq > 0))
            def _():
                lat_wait(i)

    def rope_in():
        first_half = lax.broadcasted_iota(jnp.int32, (tok, 2 * ROPE), 1) < ROPE

        def fill(slot, carry):
            rope = rope_all[slot].astype(jnp.float32)
            twice = jnp.concatenate([rope, rope], axis=0).T
            at = pl.ds(pl.multiple_of(slot * tok, tok), tok)
            for h in range(chunk_heads):
                laid = jnp.where(first_half, twice, 0.0) if h % 2 == 0 else twice
                kaug[h, at, NOPE:] = laid.astype(jnp.bfloat16)
            return carry

        lax.fori_loop(0, slots, fill, 0)

    def project(c):
        first_slot, tiles = (0, slots) if c < wide else (2 * x, look + 2)
        parts = -(-tiles // 6)
        done = 0
        for part in range(parts):
            many = (tiles - done) // (parts - part)
            slot = first_slot + done
            done += many
            block = many * tok
            at = pl.ds(pl.multiple_of(slot * tok, tok), block)
            lat = lat_all[pl.ds(slot, many)].reshape(block, rank)
            low = lax.broadcasted_iota(jnp.int32, (block, NOPE), 1) < ROPE

            def up(kv, pair):
                cols = slice(pair * 2 * NOPE, (pair + 1) * 2 * NOPE)
                return jnp.dot(
                    lat, w[c, :, kv, :, cols].reshape(rank, 2 * NOPE),
                    preferred_element_type=jnp.float32,
                )

            for pair in range(pairs):
                k = up(0, pair)
                kaug[2 * pair, at, :NOPE] = k[:, :NOPE].astype(jnp.bfloat16)
                turned = pltpu.roll(k[:, NOPE:], ROPE, axis=1)
                kaug[2 * pair + 1, at, :NOPE] = jnp.where(low, 0.0, turned).astype(jnp.bfloat16)
                rope_last = kaug[2 * pair + 1, at, NOPE:].astype(jnp.float32)
                kaug[2 * pair + 1, at, NOPE:] = jnp.where(low, turned, rope_last).astype(
                    jnp.bfloat16
                )
            for pair in range(pairs):
                v = up(1, pair)
                for side in range(2):
                    begin = (2 * pair + side) * 2 * VDIM
                    vbuf[at, begin:begin + VDIM] = v[:, side * VDIM:(side + 1) * VDIM].astype(
                        jnp.bfloat16
                    )

    scale = LOG2E / math.sqrt(QK)

    def attend(c, tiles, then):
        def places(tile):
            place_of = tile if c < wide else 2 * x + tile
            return place_of, pl.ds(pl.multiple_of(place_of * tok, tok), span)

        def scores(tile, h):
            begin = (h // 2) * 2 * QK + (h % 2) * NOPE
            return lax.dot_general(
                qbuf[c, tile, :, begin:begin + 2 * NOPE], kaug[h, places(tile)[1], :],
                (((1,), (1,)), ((), ())), preferred_element_type=jnp.float32,
            )

        def weights(tile, s):
            s = s * scale + bias[places(tile)[0]]
            peak = jnp.max(s, axis=1, keepdims=True)
            return jnp.exp2(s - peak).astype(jnp.bfloat16)

        def mix(tile, h, expo):
            both = jnp.dot(
                expo, vbuf[places(tile)[1], h * 2 * VDIM:(h + 1) * 2 * VDIM],
                preferred_element_type=jnp.float32,
            )
            given = (both[:, :VDIM] / both[:, VDIM:]).astype(jnp.bfloat16)
            obuf[c, tile, :, h * VDIM:(h + 1) * VDIM] = given

        items = [(tile, h) for tile in tiles for h in range(chunk_heads)]
        held = [scores(tile, h) for tile, h in items]
        expo = {}
        for i, (tile, h) in enumerate(items):
            expo[i] = weights(tile, held[i])
            if i > 0:
                mix(*items[i - 1], expo.pop(i - 1))
            if i == chunk_heads and c == last:
                then[0]()
        mix(*items[-1], expo.pop(len(items) - 1))
        if c != last:
            then[0]()
        then[1]()

    def q_in(c):
        landed = qbuf.at[c] if c < wide else qbuf.at[c, pl.ds(0, 2)]
        pltpu.make_async_copy(landed, landed, q_sem.at[c]).wait()

    last = order[-1][0]

    def work_on(c):
        tiles = n_head if c < wide else 2

        def pair(j):
            def keep():
                who = head if c < wide else owner(c - wide, core)
                out[:, o_cols(who, c)] = obuf[c, tile_at(c, j + 1)]

            second_sent = o_copy(c, j + 1).start if j + 2 < tiles else keep
            if j == 0:
                with jax.named_scope(f"q_in{c}"):
                    q_in(c)
            with jax.named_scope(f"work{c}_{j}"):
                if j == 0:
                    project(c)
                attend(c, [tile_at(c, j), tile_at(c, j + 1)], (o_copy(c, j).start, second_sent))

        return [(0.8, functools.partial(pair, j)) for j in range(0, tiles, 2)]

    chores = {
        (0, 1): [lat_relay],
        (1, 1): [back_relay] + [lambda c=c: start(q_copies(c)) for c in range(1, min(2, wide))]
        + [lambda k=k: x_copy(k, 0).start() for k in range(1, xs)],
        (0, 2): [back_relay_mate],
        (1, 2): [lat_done, rope_in],
    }
    chores.setdefault((wide, 1), []).extend(
        [lambda k=k: x_copy(k, 1).start() for k in range(1, xs)]
        + [lambda c=c: start(q_copies(c)) for c in range(2, wide)]
    )
    unsent, waiting, taken = order[2:], [], set()
    for c, t in order:
        with jax.named_scope(f"ring{c}_{t}"):
            ring_take(c, t)
        taken.add((c, t))
        while unsent:
            ahead, step = unsent[0]
            need = (ahead, step - 1) if step > 1 else holds.get(ahead)
            if need is not None and need not in taken:
                break
            ring_send(*unsent.pop(0))
        for chore in chores.get((c, t), []):
            with jax.named_scope("chore"):
                chore()
        if t == steps_of(c):
            waiting += work_on(c)
        room = 1.8
        while waiting and room > 0:
            cost, step = waiting.pop(0)
            step()
            room -= cost
    for _, step in waiting:
        step()

    with jax.named_scope("last"):
        landed = out.at[:, pl.ds(0, (wide * (n_head - 1) + xs) * cw)]
        pltpu.make_async_copy(landed, landed, o_sem).wait()

    with jax.named_scope("sends"):
        arrive(obuf.at[pl.ds(0, wide), pl.ds(0, n_head - 1)], o_send.at[0])
        arrive(obuf.at[pl.ds(wide, xs), pl.ds(0, 1)], o_send.at[1])
        arrive(qbuf.at[pl.ds(0, wide), pl.ds(0, n_head - 1)], q_send.at[0])
        arrive(qbuf.at[pl.ds(wide, xs), pl.ds(0, 1)], q_send.at[1])
        arrive(w.at[pl.ds(0, wide + 1), pl.ds(0, n_seq - 1)], w_send.at[0])
        arrive(w.at[pl.ds(wide + 1, xs - 1), pl.ds(0, n_seq - 2)], w_send.at[1])
        for k in range(1, xs):
            arrive(w.at[wide, pl.ds(0, 2)], x_send.at[k - 1])
        for copies in lat_out() + [lat_on(k) for k in range(1, xs)]:
            for copy in copies:
                copy.wait_send()

        @pl.when(gives)
        def _():
            for copy in back_out():
                copy.wait_send()

        @pl.when(takes)
        def _():
            for k in range(1, xs):
                for copy in back_on(k):
                    copy.wait_send()

        for i in range(look):
            @pl.when(back_side(i) & (seq > 0))
            def _():
                for copy in back_mate(i):
                    copy.wait_send()


def shards(queries, latent, rope_keys, key_weight, value_weight, doc_lengths):
    n_seq, n_head = lax.axis_size("seq"), lax.axis_size("head")
    tok, rank = latent.shape
    rows = key_weight.shape[0]
    local_heads = key_weight.shape[1] // NOPE
    docs = doc_lengths.shape[0]
    slot_rows = n_seq * n_head * tok // docs
    look = 2 * -(-slot_rows // tok) - 1
    chunk_heads = min(4, local_heads)
    wide = local_heads // chunk_heads - 1
    xs = n_head // 2
    pieces = wide + xs
    slots, span, half = look + n_head, (look + 1) * tok, n_seq // 2
    cw, qw = chunk_heads * NOPE, chunk_heads * QK
    anywhere = pl.BlockSpec(memory_space=pl.ANY)
    dma = pltpu.SemaphoreType.DMA
    bf16 = jnp.bfloat16
    return pl.pallas_call(
        functools.partial(kernel, (n_seq, n_head, look, wide, chunk_heads)),
        out_shape=pltpu.VMEM((tok, n_head * local_heads * VDIM), bf16),
        in_specs=[anywhere] * 6,
        out_specs=pl.BlockSpec(memory_space=pltpu.VMEM),
        scratch_shapes=[
            pltpu.VMEM((slots, tok, rank), bf16),
            pltpu.VMEM((slots, ROPE, tok), bf16),
            pltpu.VMEM((pieces, n_seq, 2, rows, cw), bf16),
            pltpu.VMEM((pieces, n_head, tok, qw), bf16),
            pltpu.VMEM((chunk_heads, slots * tok, 2 * NOPE), bf16),
            pltpu.VMEM((slots * tok, 2 * cw), bf16),
            pltpu.VMEM((n_head, tok, span), jnp.float32),
            pltpu.VMEM((pieces, n_head, tok, cw), bf16),
            pltpu.SMEM((docs,), jnp.int32),
            dma,
            dma((slots, 2)),
            dma((3 * xs - 1 + look, 2)),
            dma,
            dma((pieces, half)),
            dma((2,)),
            dma((xs - 1,)),
            dma((xs - 1,)),
            dma((pieces,)),
            dma((2,)),
            dma,
            dma((2,)),
        ],
        compiler_params=pltpu.CompilerParams(collective_id=0, has_side_effects=True),
    )(queries, latent, rope_keys.T, key_weight, value_weight, doc_lengths)


def solution(mesh):
    placed = (
        P(("seq", "head"), None),
        P(("seq", "head"), None),
        P(("seq", "head"), None),
        P("seq", "head"),
        P("seq", "head"),
        P(),
    )
    return jax.shard_map(
        shards, mesh=mesh, in_specs=placed, out_specs=P(("seq", "head"), None), check_vma=False
    )
```

```python
import functools
import math

import jax
import jax.numpy as jnp
from jax import lax
from jax.experimental import pallas as pl
from jax.experimental.pallas import tpu as pltpu
from jax.sharding import PartitionSpec as P

NOPE = 128
ROPE = 64
VDIM = 128
QK = NOPE + ROPE
LOG2E = 1.4426950408889634

MESH = pl.DeviceIdType.MESH


PLAN = (
    "r01", "lat", "q1", "z11", "b4", "own", "z21", "q2", "r02", "z41", "z12", "back", "z22",
    "r03", "e3", "done", "rope", "give", "qx", "z42", "i3", "z13", "z23", "r04", "w0",
    "relay", "z31", "y10", "y11", "y12", "y13", "w1", "pass", "row", "z32", "y20", "y21",
    "y22", "y23", "w2", "y40", "y41", "y42", "in", "w4", "z33", "y30", "y31", "y32", "y33",
    "w3",
)


def ring_order(pieces, wide, steps_of):
    if (pieces, wide, steps_of(0)) == (5, 3, 4):
        steps = (1, 11, 2, 12, 3, 31, 21, 13, 4, 22, 14, 32, 41, 23, 42, 24, 33, 43, 34)
        return [divmod(step, 10) for step in steps], {4: (2, 2)}
    first = [0, wide] + list(range(1, wide))
    flight, later, order = [(c, 1) for c in first[:2]], first[2:] + list(range(wide + 1, pieces)), []
    while flight:
        c, t = flight.pop(0)
        order.append((c, t))
        if t < steps_of(c):
            flight.append((c, t + 1))
        if t >= steps_of(c) // 2 and later and len(flight) < 3:
            flight.append((later.pop(0), 1))
    holds = {}
    for c in range(wide + 1, pieces):
        at = order.index((c, 1))
        holds[c] = order[max(at - 2, order.index((wide, 1)))]
    return order, holds


def kernel(
    sizes, queries, latent, rope_keys, key_weight, value_weight, lengths_in, out,
    lat_all, rope_all, w, qbuf, kaug, vbuf, bias, obuf, lengths,
    lat_ext, rope_ext, q_ext, kaug_ext, vbuf_ext, bias_ext, obuf_ext,
    z_recv, y_recv, c_send, ext_sem, ext_send, qe_sem, qe_send, oe_send,
    len_sem, lat_sem, lat_send, w_own, w_recv, w_send, x_send, x_recv, q_sem, q_send, o_sem, o_send,
):
    n_seq, n_head, look, wide, chunk_heads = sizes
    tok, rank = latent.shape
    half = n_seq // 2
    xs = n_head // 2
    slots = look + n_head
    span = (look + 1) * tok
    cw = chunk_heads * NOPE
    qw = chunk_heads * QK
    pieces = wide + xs
    q_all, o_all = (wide + 1) * qw, (wide + 1) * cw
    seq, head = lax.axis_index("seq"), lax.axis_index("head")
    core, x = head % 2, head // 2
    mate = head + 1 - 2 * core

    odd = seq % 2
    place = (seq // 2) * (1 - odd) + (n_seq - 1 - seq // 2) * odd

    def at_place(where):
        where = (where + n_seq) % n_seq
        fold = where // half
        return 2 * where * (1 - fold) + (2 * (n_seq - 1 - where) + 1) * fold

    after, before = at_place(place + 1), at_place(place - 1)

    cols = (pieces, wide, half, look) == (5, 3, 4, 1)
    z, y = seq // 2, seq % 2
    inner = (z > 0) & (z < half - 1)
    outer = jnp.logical_not(inner)
    other, ally = seq + 1 - 2 * y, seq + 2 - 4 * (z % 2)

    sides = sorted({(n_head - look + i) % 2 for i in range(look)})
    helps = (core >= 0) if len(sides) > 1 else (core == sides[0])
    gives, takes = helps & (seq < n_seq - 1), helps & (seq > 0)

    barrier = pltpu.get_barrier_semaphore()

    def greet(to_seq, to_head):
        pl.semaphore_signal(barrier, inc=1, device_id=(to_seq, to_head), device_id_type=MESH)

    greet(after, head)
    greet(before, head)
    for k in range(1, n_head):
        greet(seq, (head + k) % n_head)

    if cols:
        greet(other, head)
        greet(ally, mate)

    @pl.when(gives)
    def _():
        greet(seq + 1, head)

    @pl.when(takes)
    def _():
        greet(seq - 1, head)

    def owner(k, side):
        return ((x + k) % xs) * 2 + side

    def q_cols(who, c):
        return pl.ds(pl.multiple_of(who * q_all + c * qw, 128), qw)

    def own_copies():
        for c in range(wide + 1):
            for kv, source in enumerate((key_weight, value_weight)):
                pltpu.make_async_copy(
                    source.at[:, pl.ds(c * cw, cw)], w.at[c, seq, kv], w_own
                ).start()
        mine = look + head
        pltpu.make_async_copy(latent, lat_all.at[mine], lat_sem.at[mine, 0]).start()
        pltpu.make_async_copy(rope_keys, rope_all.at[mine], lat_sem.at[mine, 1]).start()
        for c in range(wide):
            pltpu.make_async_copy(
                queries.at[:, q_cols(head, c)], qbuf.at[c, head], q_sem.at[c]
            ).start()
        for k in range(xs):
            mine_too = pltpu.make_async_copy(
                queries.at[:, q_cols(owner(k, core), wide)],
                qbuf.at[wide + k, core], q_sem.at[wide + k],
            )
            if cols and k > 0:
                pl.when(inner)(mine_too.start)
            else:
                mine_too.start()

    own_copies()
    pltpu.make_async_copy(lengths_in, lengths, len_sem).start()
    with jax.named_scope("barrier"):
        pl.semaphore_wait(
            barrier,
            n_head + 1 + 2 * cols + gives.astype(jnp.int32) + takes.astype(jnp.int32),
        )

    def lat_copies(index, slot, to, landing):
        return [
            pltpu.make_async_remote_copy(
                src_ref=held.at[slot], dst_ref=held.at[landing],
                send_sem=lat_send.at[index, part], recv_sem=lat_sem.at[landing, part],
                device_id=to, device_id_type=MESH,
            )
            for part, held in enumerate((lat_all, rope_all))
        ]

    def lat_wait(slot):
        for part, held in enumerate((lat_all, rope_all)):
            pltpu.make_async_copy(held.at[slot], held.at[slot], lat_sem.at[slot, part]).wait()

    mine = look + head

    def lat_out():
        sent = [lat_copies(k - 1, mine, (seq, owner(k, core)), mine) for k in range(1, xs)]
        return sent + [lat_copies(xs - 1, mine, (seq, mate), mine)]

    def lat_on(k):
        slot = look + owner(k, core)
        return lat_copies(xs + look + k - 1, slot, (seq, mate), slot)

    def back_out(i):
        return lat_copies(xs + i, n_head + i, (seq + 1, head), i)

    def back_mate(i):
        return lat_copies(2 * xs + look - 1 + i, i, (seq, mate), i)

    def back_side(i):
        return core == (n_head - look + i) % 2

    def start(copies):
        for copy in copies:
            copy.start()

    def x_copy(k, near):
        rows_of = seq if near == 0 else before
        return pltpu.make_async_remote_copy(
            src_ref=w.at[wide, rows_of], dst_ref=w.at[wide + k, rows_of],
            send_sem=x_send.at[k - 1], recv_sem=x_recv.at[k - 1],
            device_id=(seq, owner(xs - k, core)), device_id_type=MESH,
        )

    def arrive(ref, sem):
        pltpu.make_async_copy(ref, ref, sem).wait()

    def steps_of(c):
        return half if c <= wide else half - 1

    def origin_at(c, t, way):
        return at_place(place - t - (c > wide)) if way == 0 else at_place(place + t)

    pairs = chunk_heads // 2

    def ring_copy(c, t, way):
        origin = origin_at(c, t - 1, way)
        block = w.at[c, origin, way] if t == half else w.at[c, origin]
        return pltpu.make_async_remote_copy(
            src_ref=block, dst_ref=block, send_sem=w_send.at[0 if c <= wide else 1],
            recv_sem=w_recv.at[c, t - 1],
            device_id=(after if way == 0 else before, head), device_id_type=MESH,
        )

    def ring_send(c, t):
        if t == 1 and c > wide:
            arrive(w.at[c, pl.ds(0, 2)], x_recv.at[c - wide - 1])
        for way in range(2):
            ring_copy(c, t, way).start()

    def ring_take(c, t):
        arrive(w.at[c, 0] if t == half else w.at[c, pl.ds(0, 2)], w_recv.at[c, t - 1])

    pairs = chunk_heads // 2

    def q_copies(c):
        if c < wide:
            routes = [((head + k) % n_head,) * 2 + (head,) for k in range(1, n_head)]
        else:
            routes = [(mate, owner(c - wide, 1 - core), core)]
        return [
            pltpu.make_async_remote_copy(
                src_ref=queries.at[:, q_cols(who, min(c, wide))], dst_ref=qbuf.at[c, slot],
                send_sem=q_send.at[0 if c < wide else 1], recv_sem=q_sem.at[c],
                device_id=(seq, peer), device_id_type=MESH,
            )
            for peer, who, slot in routes
        ]

    def tile_at(c, j):
        if c >= wide:
            return 1 - core if j == 0 else core
        if j < n_head - 2:
            return (2 * x + 2 + j) % n_head
        return mate if j == n_head - 2 else head

    def o_cols(who, c):
        return pl.ds(pl.multiple_of(who * o_all + min(c, wide) * cw, 128), cw)

    def o_copy(c, j):
        tile = tile_at(c, j)
        peer, who = (tile, head) if c < wide else (mate, owner(c - wide, core))
        return pltpu.make_async_remote_copy(
            src_ref=obuf.at[c, tile], dst_ref=out.at[:, o_cols(who, c)],
            send_sem=o_send.at[0 if c < wide else 1], recv_sem=o_sem,
            device_id=(seq, peer), device_id_type=MESH,
        )

    def z_copy(c, t, origin, up):
        block = w.at[c, 2 * origin + y]
        return pltpu.make_async_remote_copy(
            src_ref=block, dst_ref=block, send_sem=c_send.at[c // 3],
            recv_sem=z_recv.at[c - 1, t - 1],
            device_id=(seq + 2 * up, head), device_id_type=MESH,
        )

    def y_copy(c, t, origin):
        block = w.at[c, 2 * origin + y]
        return pltpu.make_async_remote_copy(
            src_ref=block, dst_ref=block, send_sem=c_send.at[c // 3],
            recv_sem=y_recv.at[c - 1, t],
            device_id=(other, head), device_id_type=MESH,
        )

    def column_start(c):
        if c == 4:
            arrive(w.at[c, 0], x_recv.at[0])
        pl.when(z <= (half - 3 if c == 4 else half - 2))(z_copy(c, 1, z, 1).start)
        pl.when(z >= (2 if c == 4 else 1))(z_copy(c, 1, z, -1).start)
        if c == 4:
            pl.when(inner)(y_copy(c, 0, z).start)
        else:
            y_copy(c, 0, z).start()

    def z_take(c, t):
        one, two, sem = w.at[c, 0], w.at[c, pl.ds(0, 2)], z_recv.at[c - 1, t - 1]
        far = z + 2 - 4 * (z // 2)

        def first_inner():
            arrive(two, sem)
            pl.when(z <= (1 if c == 4 else half))(z_copy(c, 2, z - 1, 1).start)
            pl.when(z >= (2 if c == 4 else 0))(z_copy(c, 2, z + 1, -1).start)
            if c == 3:
                y_copy(c, 1, half - 1 - z).start()
            else:
                y_copy(c, 1, z - 1).start()
                y_copy(c, 1, z + 1).start()

        def first_outer():
            arrive(one, sem)
            y_copy(c, 1, z + 1 - 2 * (z % 2)).start()

        def second():
            arrive(one, sem)
            if c < 4:
                pl.when(z == 1)(z_copy(c, 3, far, -1).start)
                pl.when(z == 2)(z_copy(c, 3, far, 1).start)
            y_copy(c, 2, far).start()

        def third():
            arrive(one, sem)
            y_copy(c, 3, half - 1 - z).start()

        if t == 1:
            pl.when(inner)(first_inner)
            if c < 4:
                pl.when(outer)(first_outer)
        elif t == 2 and c == 4:
            pl.when(inner)(second)
        elif t == 2:
            second()
        elif c < 4:
            pl.when(outer)(third)

    def y_take(c, t):
        one, two, sem = w.at[c, 0], w.at[c, pl.ds(0, 2)], y_recv.at[c - 1, t]
        if c == 3 and t == 0:
            pl.when(inner)(lambda: arrive(one, sem))
        elif c == 3:
            arrive(one, sem)
        elif t == 1:
            pl.when(inner)(lambda: arrive(two, sem))
            if c < 4:
                pl.when(outer)(lambda: arrive(one, sem))
        elif t == 3:
            pl.when(outer)(lambda: arrive(one, sem))
        elif c == 4:
            pl.when(inner)(lambda: arrive(one, sem))
        else:
            arrive(one, sem)

    def row_on():
        block = w.at[3, other]
        return pltpu.make_async_remote_copy(
            src_ref=block, dst_ref=block, send_sem=c_send.at[1], recv_sem=y_recv.at[2, 3],
            device_id=(ally, head), device_id_type=MESH,
        )

    def row_take():
        arrive(w.at[3, 0], y_recv.at[2, 0])
        row_on().start()

    def ext_copies(index, sources, slot, to):
        return [
            pltpu.make_async_remote_copy(
                src_ref=source, dst_ref=landing.at[slot],
                send_sem=ext_send.at[index, part], recv_sem=ext_sem.at[slot, part],
                device_id=to, device_id_type=MESH,
            )
            for part, (source, landing) in enumerate(zip(sources, (lat_ext, rope_ext)))
        ]

    def ext_wait(slot):
        arrive(lat_ext.at[slot], ext_sem.at[slot, 0])
        arrive(rope_ext.at[slot], ext_sem.at[slot, 1])

    def ext_give_own():
        start(ext_copies(0, (lat_all.at[mine], rope_all.at[mine]), 1 + core, (ally, head)))

    def ext_give_back():
        start(ext_copies(1, (lat_all.at[2 * x], rope_all.at[2 * x]), 0, (ally, head)))

    def ext_relay():
        ext_wait(1 + core)
        start(ext_copies(0, (lat_ext.at[1 + core], rope_ext.at[1 + core]), 1 + core, (seq, mate)))

    def ext_relay_back():
        ext_wait(0)
        start(ext_copies(1, (lat_ext.at[0], rope_ext.at[0]), 0, (seq, mate)))

    def ext_done():
        ext_wait(2 - core)
        pl.when(core == 1)(lambda: ext_wait(0))

    def ext_queries():
        for side in range(2):
            pltpu.make_async_remote_copy(
                src_ref=queries.at[:, q_cols(owner(1, side), wide)], dst_ref=q_ext.at[core],
                send_sem=qe_send, recv_sem=qe_sem,
                device_id=(ally, 2 * x + side), device_id_type=MESH,
            ).start()

    def ext_out(tile):
        return pltpu.make_async_remote_copy(
            src_ref=obuf_ext.at[tile], dst_ref=out.at[:, o_cols(owner(1, core), wide)],
            send_sem=oe_send, recv_sem=o_sem,
            device_id=(ally, 2 * x + tile), device_id_type=MESH,
        )

    order, holds = ring_order(pieces, wide, steps_of)
    arrive(w.at[pl.ds(0, wide + 1), 0], w_own)
    ring_send(*order[0])
    if cols:
        column_start(1)
        column_start(2)
    else:
        ring_send(*order[1])
    lat_wait(mine)
    start([copy for copies in lat_out() for copy in copies])
    if cols:
        x_copy(1, 0).start()
    start(q_copies(0))
    for c in range(wide, pieces):
        if cols and c > wide:
            pl.when(inner)(lambda: start(q_copies(c)))
        else:
            start(q_copies(c))

    docs = lengths.shape[0]

    def mask_of(group, j):
        first = group * n_head * tok
        q_place = first + j * tok + lax.broadcasted_iota(jnp.int32, (tok, 1), 0)

        def document(d, state):
            begin, begun = state
            return begin + lengths[d], jnp.where(begin <= q_place, begin, begun)

        _, begun = lax.fori_loop(
            0, docs, document, (jnp.int32(0), jnp.zeros((tok, 1), jnp.int32)), unroll=True
        )
        k_place = first + (j - look) * tok + lax.broadcasted_iota(jnp.int32, (tok, span), 1)
        seen = (k_place >= begun) & (k_place <= q_place)
        return jnp.where(seen, 0.0, -jnp.inf)

    def mask_tile(j, carry):
        bias[j] = mask_of(seq, j)
        return carry

    def mask_ext(j, carry):
        bias_ext[j] = mask_of(ally, 2 * x + j)
        return carry

    with jax.named_scope("mask"):
        pltpu.make_async_copy(lengths_in, lengths, len_sem).wait()
        lax.fori_loop(0, n_head, mask_tile, 0)
        if cols:
            @pl.when(inner)
            def _():
                lax.fori_loop(0, 2, mask_ext, 0)
                for h in range(chunk_heads):
                    vbuf_ext[:, (2 * h + 1) * VDIM:(2 * h + 2) * VDIM] = jnp.ones(
                        ((look + 2) * tok, VDIM), jnp.bfloat16
                    )

        @pl.when(seq == 0)
        def _():
            lat_all[:look] = jnp.zeros((look, tok, rank), jnp.bfloat16)
            rope_all[:look] = jnp.zeros((look, ROPE, tok), jnp.bfloat16)

        for h in range(chunk_heads):
            vbuf[:, (2 * h + 1) * VDIM:(2 * h + 2) * VDIM] = jnp.ones(
                (slots * tok, VDIM), jnp.bfloat16
            )

    def lat_relay():
        for k in range(1, xs):
            lat_wait(look + owner(k, core))
            start(lat_on(k))

        for i in range(look):
            @pl.when(back_side(i) & (seq < n_seq - 1))
            def _():
                start(back_out(i))

    def back_relay():
        for i in range(look):
            @pl.when(back_side(i) & (seq > 0))
            def _():
                lat_wait(i)
                start(back_mate(i))

    def lat_done():
        for k in range(xs):
            lat_wait(look + owner(k, 1 - core))
        for i in range(look):
            @pl.when(jnp.logical_not(back_side(i)) & (seq > 0))
            def _():
                lat_wait(i)

    def rope_in(ropes, augmented, count):
        first_half = lax.broadcasted_iota(jnp.int32, (tok, 2 * ROPE), 1) < ROPE

        def fill(slot, carry):
            rope = ropes[slot].astype(jnp.float32)
            twice = jnp.concatenate([rope, rope], axis=0).T
            at = pl.ds(pl.multiple_of(slot * tok, tok), tok)
            for h in range(chunk_heads):
                laid = jnp.where(first_half, twice, 0.0) if h % 2 == 0 else twice
                augmented[h, at, NOPE:] = laid.astype(jnp.bfloat16)
            return carry

        lax.fori_loop(0, count, fill, 0)

    def rope_own():
        rope_in(rope_all, kaug, slots)

    own_refs = (lat_all, kaug, vbuf, bias, qbuf, obuf)
    ext_refs = (lat_ext, kaug_ext, vbuf_ext, bias_ext, q_ext, obuf_ext)

    def project(c, ext):
        lat_all, kaug, vbuf = (ext_refs if ext else own_refs)[:3]
        first_slot, tiles = (0, slots) if c < wide else (0 if ext else 2 * x, look + 2)
        parts = -(-tiles // 6)
        done = 0
        for part in range(parts):
            many = (tiles - done) // (parts - part)
            slot = first_slot + done
            done += many
            block = many * tok
            at = pl.ds(pl.multiple_of(slot * tok, tok), block)
            lat = lat_all[pl.ds(slot, many)].reshape(block, rank)
            low = lax.broadcasted_iota(jnp.int32, (block, NOPE), 1) < ROPE

            def up(kv, pair):
                cols = slice(pair * 2 * NOPE, (pair + 1) * 2 * NOPE)
                return jnp.dot(
                    lat, w[c, :, kv, :, cols].reshape(rank, 2 * NOPE),
                    preferred_element_type=jnp.float32,
                )

            for pair in range(pairs):
                k = up(0, pair)
                kaug[2 * pair, at, :NOPE] = k[:, :NOPE].astype(jnp.bfloat16)
                turned = pltpu.roll(k[:, NOPE:], ROPE, axis=1)
                kaug[2 * pair + 1, at, :NOPE] = jnp.where(low, 0.0, turned).astype(jnp.bfloat16)
                rope_last = kaug[2 * pair + 1, at, NOPE:].astype(jnp.float32)
                kaug[2 * pair + 1, at, NOPE:] = jnp.where(low, turned, rope_last).astype(
                    jnp.bfloat16
                )
            for pair in range(pairs):
                v = up(1, pair)
                for side in range(2):
                    begin = (2 * pair + side) * 2 * VDIM
                    vbuf[at, begin:begin + VDIM] = v[:, side * VDIM:(side + 1) * VDIM].astype(
                        jnp.bfloat16
                    )

    scale = LOG2E / math.sqrt(QK)

    def attend(c, tiles, then, ext):
        _, kaug, vbuf, bias, queries_in, given_out = ext_refs if ext else own_refs
        if not ext:
            queries_in, given_out = qbuf.at[c], obuf.at[c]

        def places(tile):
            place_of = tile if c < wide or ext else 2 * x + tile
            return place_of, pl.ds(pl.multiple_of(place_of * tok, tok), span)

        def scores(tile, h):
            begin = (h // 2) * 2 * QK + (h % 2) * NOPE
            return lax.dot_general(
                queries_in[tile, :, begin:begin + 2 * NOPE], kaug[h, places(tile)[1], :],
                (((1,), (1,)), ((), ())), preferred_element_type=jnp.float32,
            )

        def weights(tile, s):
            s = s * scale + bias[places(tile)[0]]
            peak = jnp.max(s, axis=1, keepdims=True)
            return jnp.exp2(s - peak).astype(jnp.bfloat16)

        def mix(tile, h, expo):
            both = jnp.dot(
                expo, vbuf[places(tile)[1], h * 2 * VDIM:(h + 1) * 2 * VDIM],
                preferred_element_type=jnp.float32,
            )
            given = (both[:, :VDIM] / both[:, VDIM:]).astype(jnp.bfloat16)
            given_out[tile, :, h * VDIM:(h + 1) * VDIM] = given

        items = [(tile, h) for tile in tiles for h in range(chunk_heads)]
        held = [scores(tile, h) for tile, h in items]
        expo = {}
        for i, (tile, h) in enumerate(items):
            expo[i] = weights(tile, held[i])
            if i > 0:
                mix(*items[i - 1], expo.pop(i - 1))
            if i == chunk_heads and c == last and not ext:
                then[0]()
        mix(*items[-1], expo.pop(len(items) - 1))
        if c != last or ext:
            then[0]()
        then[1]()

    def q_in(c):
        landed = qbuf.at[c] if c < wide else qbuf.at[c, pl.ds(0, 2)]
        pltpu.make_async_copy(landed, landed, q_sem.at[c]).wait()

    last = wide if cols else order[-1][0]

    def work_on(c):
        tiles = n_head if c < wide else 2

        def pair(j):
            def keep():
                who = head if c < wide else owner(c - wide, core)
                out[:, o_cols(who, c)] = obuf[c, tile_at(c, j + 1)]

            second_sent = o_copy(c, j + 1).start if j + 2 < tiles else keep
            if j == 0:
                with jax.named_scope(f"q_in{c}"):
                    q_in(c)
            with jax.named_scope(f"work{c}_{j}"):
                if j == 0:
                    project(c, False)
                attend(c, [tile_at(c, j), tile_at(c, j + 1)], (o_copy(c, j).start, second_sent), False)

        def ally_pair():
            arrive(q_ext, qe_sem)
            project(c, True)
            attend(c, [0, 1], (ext_out(0).start, ext_out(1).start), True)

        if cols and c > wide:
            return [
                (0.8, lambda: pl.when(inner)(lambda: pair(0))),
                (0.8, lambda: pl.when(inner)(ally_pair)),
            ]
        return [(0.8, functools.partial(pair, j)) for j in range(0, tiles, 2)]

    def column_plan():
        def only_inner(work):
            return lambda: pl.when(inner)(work)

        def only_outer(work):
            return lambda: pl.when(outer)(work)

        def ext_in():
            ext_done()
            rope_in(rope_ext, kaug_ext, look + 2)

        def back():
            pl.when(outer & (core == 0))(ext_give_back)

        def relay_back():
            pl.when(inner & (core == 0))(ext_relay_back)

        steps = {"r": ring_step, "z": z_take, "y": y_take}
        plan = PLAN
        todo = {
            "lat": lat_relay, "q1": lambda: start(q_copies(1)), "q2": lambda: start(q_copies(2)),
            "qx": only_outer(ext_queries), "back": back_relay, "done": lat_done,
            "rope": rope_own, "give": back, "own": only_outer(ext_give_own),
            "e3": only_outer(lambda: column_start(3)),
            "i3": only_inner(lambda: column_start(3)),
            "row": only_outer(row_take), "relay": only_inner(ext_relay), "pass": relay_back,
            "in": only_inner(ext_in),
        }
        waiting = []
        for step in plan:
            kind, rest = step[0], step[1:]
            with jax.named_scope(step):
                if step in todo:
                    todo[step]()
                elif kind == "b":
                    column_start(int(rest))
                elif kind == "w":
                    waiting += work_on(int(rest))
                else:
                    steps[kind](int(rest[0]), int(rest[1]))
            room = 1.8 if kind in "rzyw" else 0
            while waiting and room > 0:
                cost, work = waiting.pop(0)
                work()
                room -= cost
        for _, work in waiting:
            work()

    def ring_step(c, t):
        ring_take(c, t)
        if t < half:
            ring_send(c, t + 1)

    def ring_plan():
        chores = {
            (0, 1): [lat_relay],
            (1, 1): [lambda c=c: start(q_copies(c)) for c in range(1, min(2, wide))]
            + [lambda k=k: x_copy(k, 0).start() for k in range(1, xs)],
            (0, min(3, half - 1)): [back_relay],
        }
        chores.setdefault(order[order.index((0, half)) - 1], []).extend([lat_done, rope_own])
        chores.setdefault((wide, 1), []).extend(
            [lambda k=k: x_copy(k, 1).start() for k in range(1, xs)]
            + [lambda c=c: start(q_copies(c)) for c in range(2, wide)]
        )
        unsent, waiting, taken = order[2:], [], set()
        for c, t in order:
            with jax.named_scope(f"ring{c}_{t}"):
                ring_take(c, t)
            taken.add((c, t))
            while unsent:
                ahead, step = unsent[0]
                need = (ahead, step - 1) if step > 1 else holds.get(ahead)
                if need is not None and need not in taken:
                    break
                ring_send(*unsent.pop(0))
            for chore in chores.get((c, t), []):
                with jax.named_scope("chore"):
                    chore()
            if t == steps_of(c):
                waiting += work_on(c)
            room = 1.8
            while waiting and room > 0:
                cost, step = waiting.pop(0)
                step()
                room -= cost
        for _, step in waiting:
            step()

    if cols:
        column_plan()
    else:
        ring_plan()

    with jax.named_scope("last"):
        def outs(many):
            arrive(out.at[:, pl.ds(0, (wide * (n_head - 1) + many) * cw)], o_sem)

        if cols:
            pl.when(inner)(lambda: outs(xs))
            pl.when(outer)(lambda: outs(xs + 1))
        else:
            outs(xs)

    with jax.named_scope("sends"):
        arrive(obuf.at[pl.ds(0, wide), pl.ds(0, n_head - 1)], o_send.at[0])
        arrive(qbuf.at[pl.ds(0, wide), pl.ds(0, n_head - 1)], q_send.at[0])

        def local_sent(many):
            arrive(obuf.at[pl.ds(wide, many), pl.ds(0, 1)], o_send.at[1])
            arrive(qbuf.at[pl.ds(wide, many), pl.ds(0, 1)], q_send.at[1])

        if cols:
            arrive(w.at[0, pl.ds(0, n_seq - 1)], w_send.at[0])
            arrive(w.at[0, 0], x_send.at[0])

            def inner_sent():
                local_sent(2)
                arrive(w.at[pl.ds(0, 3), pl.ds(0, 6)], c_send.at[0])
                arrive(w.at[pl.ds(0, 2), pl.ds(0, 7)], c_send.at[1])
                arrive(obuf_ext, oe_send)

            def outer_sent():
                local_sent(1)
                arrive(w.at[pl.ds(0, 2), pl.ds(0, 5)], c_send.at[0])
                arrive(w.at[0, pl.ds(0, 7)], c_send.at[1])
                arrive(q_ext, qe_send)

            pl.when(inner)(inner_sent)
            pl.when(outer)(outer_sent)

            def ext_sent(index):
                arrive(lat_ext.at[0], ext_send.at[index, 0])
                arrive(rope_ext.at[0], ext_send.at[index, 1])

            ext_sent(0)
            pl.when(core == 0)(lambda: ext_sent(1))
        else:
            local_sent(xs)
            arrive(w.at[pl.ds(0, wide + 1), pl.ds(0, n_seq - 1)], w_send.at[0])
            arrive(w.at[pl.ds(wide + 1, xs - 1), pl.ds(0, n_seq - 2)], w_send.at[1])
            for k in range(1, xs):
                arrive(w.at[wide, pl.ds(0, 2)], x_send.at[k - 1])
        for copies in lat_out() + [lat_on(k) for k in range(1, xs)]:
            for copy in copies:
                copy.wait_send()

        for i in range(look):
            @pl.when(back_side(i) & (seq < n_seq - 1))
            def _():
                for copy in back_out(i):
                    copy.wait_send()

            @pl.when(back_side(i) & (seq > 0))
            def _():
                for copy in back_mate(i):
                    copy.wait_send()


def shards(queries, latent, rope_keys, key_weight, value_weight, doc_lengths):
    n_seq, n_head = lax.axis_size("seq"), lax.axis_size("head")
    tok, rank = latent.shape
    rows = key_weight.shape[0]
    local_heads = key_weight.shape[1] // NOPE
    docs = doc_lengths.shape[0]
    slot_rows = n_seq * n_head * tok // docs
    look = 2 * -(-slot_rows // tok) - 1
    chunk_heads = min(4, local_heads)
    wide = local_heads // chunk_heads - 1
    xs = n_head // 2
    pieces = wide + xs
    slots, span, half = look + n_head, (look + 1) * tok, n_seq // 2
    cw, qw = chunk_heads * NOPE, chunk_heads * QK
    anywhere = pl.BlockSpec(memory_space=pl.ANY)
    dma = pltpu.SemaphoreType.DMA
    bf16 = jnp.bfloat16
    return pl.pallas_call(
        functools.partial(kernel, (n_seq, n_head, look, wide, chunk_heads)),
        out_shape=pltpu.VMEM((tok, n_head * local_heads * VDIM), bf16),
        in_specs=[anywhere] * 6,
        out_specs=pl.BlockSpec(memory_space=pltpu.VMEM),
        scratch_shapes=[
            pltpu.VMEM((slots, tok, rank), bf16),
            pltpu.VMEM((slots, ROPE, tok), bf16),
            pltpu.VMEM((pieces, n_seq, 2, rows, cw), bf16),
            pltpu.VMEM((pieces, n_head, tok, qw), bf16),
            pltpu.VMEM((chunk_heads, slots * tok, 2 * NOPE), bf16),
            pltpu.VMEM((slots * tok, 2 * cw), bf16),
            pltpu.VMEM((n_head, tok, span), jnp.float32),
            pltpu.VMEM((pieces, n_head, tok, cw), bf16),
            pltpu.SMEM((docs,), jnp.int32),
            pltpu.VMEM((look + 2, tok, rank), bf16),
            pltpu.VMEM((look + 2, ROPE, tok), bf16),
            pltpu.VMEM((2, tok, qw), bf16),
            pltpu.VMEM((chunk_heads, (look + 2) * tok, 2 * NOPE), bf16),
            pltpu.VMEM(((look + 2) * tok, 2 * cw), bf16),
            pltpu.VMEM((2, tok, span), jnp.float32),
            pltpu.VMEM((2, tok, cw), bf16),
            dma((4, 3)),
            dma((4, 4)),
            dma((2,)),
            dma((look + 2, 2)),
            dma((2, 2)),
            dma,
            dma,
            dma,
            dma,
            dma((slots, 2)),
            dma((2 * xs - 1 + 2 * look, 2)),
            dma,
            dma((1 if (pieces, wide, half, look) == (5, 3, 4, 1) else pieces, half)),
            dma((2,)),
            dma((xs - 1,)),
            dma((xs - 1,)),
            dma((pieces,)),
            dma((2,)),
            dma,
            dma((2,)),
        ],
        compiler_params=pltpu.CompilerParams(collective_id=0, has_side_effects=True),
    )(queries, latent, rope_keys.T, key_weight, value_weight, doc_lengths)


def solution(mesh):
    placed = (
        P(("seq", "head"), None),
        P(("seq", "head"), None),
        P(("seq", "head"), None),
        P("seq", "head"),
        P("seq", "head"),
        P(),
    )
    return jax.shard_map(
        shards, mesh=mesh, in_specs=placed, out_specs=P(("seq", "head"), None), check_vma=False
    )
```

```python
import functools
import math

import jax
import jax.numpy as jnp
from jax import lax
from jax.experimental import pallas as pl
from jax.experimental.pallas import tpu as pltpu
from jax.sharding import PartitionSpec as P

NOPE = 128
ROPE = 64
VDIM = 128
QK = NOPE + ROPE
LOG2E = 1.4426950408889634

MESH = pl.DeviceIdType.MESH


PLAN = (
    "r01", "lat", "q1", "z11", "b4", "own", "z21", "q2", "r02", "z41", "z12", "back", "z22",
    "r03", "e3", "done", "rope", "give", "qx", "z42", "i3", "z13", "z23", "r04", "w0",
    "relay", "z31", "y1", "w1", "pass", "row", "z32", "y2", "w2", "y4", "in", "w4", "z33",
    "y3", "w3",
)


def ring_order(pieces, wide, steps_of):
    if (pieces, wide, steps_of(0)) == (5, 3, 4):
        steps = (1, 11, 2, 12, 3, 31, 21, 13, 4, 22, 14, 32, 41, 23, 42, 24, 33, 43, 34)
        return [divmod(step, 10) for step in steps], {4: (2, 2)}
    first = [0, wide] + list(range(1, wide))
    flight, later, order = [(c, 1) for c in first[:2]], first[2:] + list(range(wide + 1, pieces)), []
    while flight:
        c, t = flight.pop(0)
        order.append((c, t))
        if t < steps_of(c):
            flight.append((c, t + 1))
        if t >= steps_of(c) // 2 and later and len(flight) < 3:
            flight.append((later.pop(0), 1))
    holds = {}
    for c in range(wide + 1, pieces):
        at = order.index((c, 1))
        holds[c] = order[max(at - 2, order.index((wide, 1)))]
    return order, holds


def kernel(
    sizes, queries, latent, rope_keys, key_weight, value_weight, lengths_in, out,
    lat_all, rope_all, w, qbuf, kaug, vbuf, bias, obuf, lengths,
    lat_ext, rope_ext, q_ext, kaug_ext, vbuf_ext, bias_ext, obuf_ext,
    z_recv, y_recv, c_send, ext_sem, ext_send, qe_sem, qe_send, oe_send,
    len_sem, lat_sem, lat_send, w_own, w_recv, w_send, x_send, x_recv, q_sem, q_send, o_sem, o_send,
):
    n_seq, n_head, look, wide, chunk_heads = sizes
    tok, rank = latent.shape
    half = n_seq // 2
    xs = n_head // 2
    slots = look + n_head
    span = (look + 1) * tok
    cw = chunk_heads * NOPE
    qw = chunk_heads * QK
    pieces = wide + xs
    q_all, o_all = (wide + 1) * qw, (wide + 1) * cw
    seq, head = lax.axis_index("seq"), lax.axis_index("head")
    core, x = head % 2, head // 2
    mate = head + 1 - 2 * core

    odd = seq % 2
    place = (seq // 2) * (1 - odd) + (n_seq - 1 - seq // 2) * odd

    def at_place(where):
        where = (where + n_seq) % n_seq
        fold = where // half
        return 2 * where * (1 - fold) + (2 * (n_seq - 1 - where) + 1) * fold

    after, before = at_place(place + 1), at_place(place - 1)

    cols = (pieces, wide, half, look) == (5, 3, 4, 1)
    z, y = seq // 2, seq % 2
    inner = (z > 0) & (z < half - 1)
    outer = jnp.logical_not(inner)
    other, ally = seq + 1 - 2 * y, seq + 2 - 4 * (z % 2)

    sides = sorted({(n_head - look + i) % 2 for i in range(look)})
    helps = (core >= 0) if len(sides) > 1 else (core == sides[0])
    gives, takes = helps & (seq < n_seq - 1), helps & (seq > 0)

    barrier = pltpu.get_barrier_semaphore()

    def greet(to_seq, to_head):
        pl.semaphore_signal(barrier, inc=1, device_id=(to_seq, to_head), device_id_type=MESH)

    greet(after, head)
    greet(before, head)
    for k in range(1, n_head):
        greet(seq, (head + k) % n_head)

    if cols:
        greet(other, head)
        greet(ally, mate)

    @pl.when(gives)
    def _():
        greet(seq + 1, head)

    @pl.when(takes)
    def _():
        greet(seq - 1, head)

    def owner(k, side):
        return ((x + k) % xs) * 2 + side

    def q_cols(who, c):
        return pl.ds(pl.multiple_of(who * q_all + c * qw, 128), qw)

    def own_copies():
        for c in range(wide + 1):
            for kv, source in enumerate((key_weight, value_weight)):
                pltpu.make_async_copy(
                    source.at[:, pl.ds(c * cw, cw)], w.at[c, seq, kv], w_own
                ).start()
        mine = look + head
        pltpu.make_async_copy(latent, lat_all.at[mine], lat_sem.at[mine, 0]).start()
        pltpu.make_async_copy(rope_keys, rope_all.at[mine], lat_sem.at[mine, 1]).start()
        for c in range(wide):
            pltpu.make_async_copy(
                queries.at[:, q_cols(head, c)], qbuf.at[c, head], q_sem.at[c]
            ).start()
        for k in range(xs):
            mine_too = pltpu.make_async_copy(
                queries.at[:, q_cols(owner(k, core), wide)],
                qbuf.at[wide + k, core], q_sem.at[wide + k],
            )
            if cols and k > 0:
                pl.when(inner)(mine_too.start)
            else:
                mine_too.start()

    own_copies()
    pltpu.make_async_copy(lengths_in, lengths, len_sem).start()
    with jax.named_scope("barrier"):
        pl.semaphore_wait(
            barrier,
            n_head + 1 + 2 * cols + gives.astype(jnp.int32) + takes.astype(jnp.int32),
        )

    def lat_copies(index, slot, to, landing):
        return [
            pltpu.make_async_remote_copy(
                src_ref=held.at[slot], dst_ref=held.at[landing],
                send_sem=lat_send.at[index, part], recv_sem=lat_sem.at[landing, part],
                device_id=to, device_id_type=MESH,
            )
            for part, held in enumerate((lat_all, rope_all))
        ]

    def lat_wait(slot):
        for part, held in enumerate((lat_all, rope_all)):
            pltpu.make_async_copy(held.at[slot], held.at[slot], lat_sem.at[slot, part]).wait()

    mine = look + head

    def lat_out():
        sent = [lat_copies(0, mine, (seq, owner(k, core)), mine) for k in range(1, xs)]
        return sent + [lat_copies(0, mine, (seq, mate), mine)]

    def lat_on(k):
        slot = look + owner(k, core)
        return lat_copies(0, slot, (seq, mate), slot)

    def back_out(i):
        return lat_copies(1 + i, n_head + i, (seq + 1, head), i)

    def back_mate(i):
        return lat_copies(1 + look + i, i, (seq, mate), i)

    def back_side(i):
        return core == (n_head - look + i) % 2

    def start(copies):
        for copy in copies:
            copy.start()

    def x_copy(k, near):
        rows_of = seq if near == 0 else before
        return pltpu.make_async_remote_copy(
            src_ref=w.at[wide, rows_of], dst_ref=w.at[wide + k, rows_of],
            send_sem=x_send.at[k - 1], recv_sem=x_recv.at[k - 1],
            device_id=(seq, owner(xs - k, core)), device_id_type=MESH,
        )

    def arrive(ref, sem):
        pltpu.make_async_copy(ref, ref, sem).wait()

    def steps_of(c):
        return half if c <= wide else half - 1

    def origin_at(c, t, way):
        return at_place(place - t - (c > wide)) if way == 0 else at_place(place + t)

    pairs = chunk_heads // 2

    def ring_copy(c, t, way):
        origin = origin_at(c, t - 1, way)
        block = w.at[c, origin, way] if t == half else w.at[c, origin]
        return pltpu.make_async_remote_copy(
            src_ref=block, dst_ref=block, send_sem=w_send.at[0 if c <= wide else 1],
            recv_sem=w_recv.at[c, t - 1],
            device_id=(after if way == 0 else before, head), device_id_type=MESH,
        )

    def ring_send(c, t):
        if t == 1 and c > wide:
            arrive(w.at[c, pl.ds(0, 2)], x_recv.at[c - wide - 1])
        for way in range(2):
            ring_copy(c, t, way).start()

    def ring_take(c, t):
        arrive(w.at[c, 0] if t == half else w.at[c, pl.ds(0, 2)], w_recv.at[c, t - 1])

    pairs = chunk_heads // 2

    def q_copies(c):
        if c < wide:
            routes = [((head + k) % n_head,) * 2 + (head,) for k in range(1, n_head)]
        else:
            routes = [(mate, owner(c - wide, 1 - core), core)]
        return [
            pltpu.make_async_remote_copy(
                src_ref=queries.at[:, q_cols(who, min(c, wide))], dst_ref=qbuf.at[c, slot],
                send_sem=q_send.at[0 if c < wide else 1], recv_sem=q_sem.at[c],
                device_id=(seq, peer), device_id_type=MESH,
            )
            for peer, who, slot in routes
        ]

    def tile_at(c, j):
        if c >= wide:
            return 1 - core if j == 0 else core
        if j < n_head - 2:
            return (2 * x + 2 + j) % n_head
        return mate if j == n_head - 2 else head

    def o_cols(who, c):
        return pl.ds(pl.multiple_of(who * o_all + min(c, wide) * cw, 128), cw)

    def o_copy(c, j):
        tile = tile_at(c, j)
        peer, who = (tile, head) if c < wide else (mate, owner(c - wide, core))
        return pltpu.make_async_remote_copy(
            src_ref=obuf.at[c, tile], dst_ref=out.at[:, o_cols(who, c)],
            send_sem=o_send.at[0 if c < wide else 1], recv_sem=o_sem,
            device_id=(seq, peer), device_id_type=MESH,
        )

    def z_copy(c, t, origin, up):
        block = w.at[c, 2 * origin + y]
        return pltpu.make_async_remote_copy(
            src_ref=block, dst_ref=block, send_sem=c_send.at[c // 3],
            recv_sem=z_recv.at[c - 1, t - 1],
            device_id=(seq + 2 * up, head), device_id_type=MESH,
        )

    def y_copy(c, t, origin):
        block = w.at[c, 2 * origin + y]
        return pltpu.make_async_remote_copy(
            src_ref=block, dst_ref=block, send_sem=c_send.at[c // 3],
            recv_sem=y_recv.at[4 if c == 3 and t == 0 else c - 1],
            device_id=(other, head), device_id_type=MESH,
        )

    def column_start(c):
        if c == 4:
            arrive(w.at[c, 0], x_recv.at[0])
        pl.when(z <= (half - 3 if c == 4 else half - 2))(z_copy(c, 1, z, 1).start)
        pl.when(z >= (2 if c == 4 else 1))(z_copy(c, 1, z, -1).start)
        if c == 4:
            pl.when(inner)(y_copy(c, 0, z).start)
        else:
            y_copy(c, 0, z).start()

    def z_take(c, t):
        one, two, sem = w.at[c, 0], w.at[c, pl.ds(0, 2)], z_recv.at[c - 1, t - 1]
        far = z + 2 - 4 * (z // 2)

        def first_inner():
            arrive(two, sem)
            pl.when(z <= (1 if c == 4 else half))(z_copy(c, 2, z - 1, 1).start)
            pl.when(z >= (2 if c == 4 else 0))(z_copy(c, 2, z + 1, -1).start)
            if c == 3:
                y_copy(c, 1, half - 1 - z).start()
            else:
                y_copy(c, 1, z - 1).start()
                y_copy(c, 1, z + 1).start()

        def first_outer():
            arrive(one, sem)
            y_copy(c, 1, z + 1 - 2 * (z % 2)).start()

        def second():
            arrive(one, sem)
            if c < 4:
                pl.when(z == 1)(z_copy(c, 3, far, -1).start)
                pl.when(z == 2)(z_copy(c, 3, far, 1).start)
            y_copy(c, 2, far).start()

        def third():
            arrive(one, sem)
            y_copy(c, 3, half - 1 - z).start()

        if t == 1:
            pl.when(inner)(first_inner)
            if c < 4:
                pl.when(outer)(first_outer)
        elif t == 2 and c == 4:
            pl.when(inner)(second)
        elif t == 2:
            second()
        elif c < 4:
            pl.when(outer)(third)

    def y_take(c):
        def whole():
            arrive(w.at[c, pl.ds(0, 4)], y_recv.at[c - 1])

        if c == 3:
            pl.when(inner)(lambda: arrive(w.at[c, 0], y_recv.at[4]))
            arrive(w.at[c, pl.ds(0, 3)], y_recv.at[c - 1])
        elif c == 4:
            pl.when(inner)(whole)
        else:
            whole()

    def row_on():
        block = w.at[3, other]
        return pltpu.make_async_remote_copy(
            src_ref=block, dst_ref=block, send_sem=c_send.at[1], recv_sem=y_recv.at[2],
            device_id=(ally, head), device_id_type=MESH,
        )

    def row_take():
        arrive(w.at[3, 0], y_recv.at[4])
        row_on().start()

    def ext_copies(index, sources, slot, to):
        return [
            pltpu.make_async_remote_copy(
                src_ref=source, dst_ref=landing.at[slot],
                send_sem=ext_send.at[index, part], recv_sem=ext_sem.at[slot, part],
                device_id=to, device_id_type=MESH,
            )
            for part, (source, landing) in enumerate(zip(sources, (lat_ext, rope_ext)))
        ]

    def ext_wait(slot):
        arrive(lat_ext.at[slot], ext_sem.at[slot, 0])
        arrive(rope_ext.at[slot], ext_sem.at[slot, 1])

    def ext_give_own():
        start(ext_copies(0, (lat_all.at[mine], rope_all.at[mine]), 1 + core, (ally, head)))

    def ext_give_back():
        start(ext_copies(1, (lat_all.at[2 * x], rope_all.at[2 * x]), 0, (ally, head)))

    def ext_relay():
        ext_wait(1 + core)
        start(ext_copies(0, (lat_ext.at[1 + core], rope_ext.at[1 + core]), 1 + core, (seq, mate)))

    def ext_relay_back():
        ext_wait(0)
        start(ext_copies(1, (lat_ext.at[0], rope_ext.at[0]), 0, (seq, mate)))

    def ext_done():
        ext_wait(2 - core)
        pl.when(core == 1)(lambda: ext_wait(0))

    def ext_queries():
        for side in range(2):
            pltpu.make_async_remote_copy(
                src_ref=queries.at[:, q_cols(owner(1, side), wide)], dst_ref=q_ext.at[core],
                send_sem=qe_send, recv_sem=qe_sem,
                device_id=(ally, 2 * x + side), device_id_type=MESH,
            ).start()

    def ext_out(tile):
        return pltpu.make_async_remote_copy(
            src_ref=obuf_ext.at[tile], dst_ref=out.at[:, o_cols(owner(1, core), wide)],
            send_sem=oe_send, recv_sem=o_sem,
            device_id=(ally, 2 * x + tile), device_id_type=MESH,
        )

    order, holds = ring_order(pieces, wide, steps_of)
    arrive(w.at[pl.ds(0, wide + 1), 0], w_own)
    lat_wait(mine)
    start([copy for copies in lat_out() for copy in copies])
    if cols:
        x_copy(1, 0).start()
    ring_send(*order[0])
    if cols:
        column_start(1)
        column_start(2)
    else:
        ring_send(*order[1])
    start(q_copies(0))
    for c in range(wide, pieces):
        if cols and c > wide:
            pl.when(inner)(lambda: start(q_copies(c)))
        else:
            start(q_copies(c))

    docs = lengths.shape[0]

    def mask_of(group, j):
        first = group * n_head * tok
        q_place = first + j * tok + lax.broadcasted_iota(jnp.int32, (tok, 1), 0)

        def document(d, state):
            begin, begun = state
            return begin + lengths[d], jnp.where(begin <= q_place, begin, begun)

        _, begun = lax.fori_loop(
            0, docs, document, (jnp.int32(0), jnp.zeros((tok, 1), jnp.int32)), unroll=True
        )
        k_place = first + (j - look) * tok + lax.broadcasted_iota(jnp.int32, (tok, span), 1)
        seen = (k_place >= begun) & (k_place <= q_place)
        return jnp.where(seen, 0.0, -jnp.inf)

    def mask_tile(j, carry):
        bias[j] = mask_of(seq, j)
        return carry

    def mask_ext(j, carry):
        bias_ext[j] = mask_of(ally, 2 * x + j)
        return carry

    with jax.named_scope("mask"):
        pltpu.make_async_copy(lengths_in, lengths, len_sem).wait()
        lax.fori_loop(0, n_head, mask_tile, 0)
        if cols:
            @pl.when(inner)
            def _():
                lax.fori_loop(0, 2, mask_ext, 0)
                for h in range(chunk_heads):
                    vbuf_ext[:, (2 * h + 1) * VDIM:(2 * h + 2) * VDIM] = jnp.ones(
                        ((look + 2) * tok, VDIM), jnp.bfloat16
                    )

        @pl.when(seq == 0)
        def _():
            lat_all[:look] = jnp.zeros((look, tok, rank), jnp.bfloat16)
            rope_all[:look] = jnp.zeros((look, ROPE, tok), jnp.bfloat16)

        for h in range(chunk_heads):
            vbuf[:, (2 * h + 1) * VDIM:(2 * h + 2) * VDIM] = jnp.ones(
                (slots * tok, VDIM), jnp.bfloat16
            )

    def lat_relay():
        for k in range(1, xs):
            lat_wait(look + owner(k, core))
            start(lat_on(k))

        for i in range(look):
            @pl.when(back_side(i) & (seq < n_seq - 1))
            def _():
                start(back_out(i))

    def back_relay():
        for i in range(look):
            @pl.when(back_side(i) & (seq > 0))
            def _():
                lat_wait(i)
                start(back_mate(i))

    def lat_done():
        for k in range(xs):
            lat_wait(look + owner(k, 1 - core))
        for i in range(look):
            @pl.when(jnp.logical_not(back_side(i)) & (seq > 0))
            def _():
                lat_wait(i)

    def rope_in(ropes, augmented, count):
        first_half = lax.broadcasted_iota(jnp.int32, (tok, 2 * ROPE), 1) < ROPE

        def fill(slot, carry):
            rope = ropes[slot].astype(jnp.float32)
            twice = jnp.concatenate([rope, rope], axis=0).T
            at = pl.ds(pl.multiple_of(slot * tok, tok), tok)
            for h in range(chunk_heads):
                laid = jnp.where(first_half, twice, 0.0) if h % 2 == 0 else twice
                augmented[h, at, NOPE:] = laid.astype(jnp.bfloat16)
            return carry

        lax.fori_loop(0, count, fill, 0)

    def rope_own():
        rope_in(rope_all, kaug, slots)

    own_refs = (lat_all, kaug, vbuf, bias, qbuf, obuf)
    ext_refs = (lat_ext, kaug_ext, vbuf_ext, bias_ext, q_ext, obuf_ext)

    def project(c, ext):
        lat_all, kaug, vbuf = (ext_refs if ext else own_refs)[:3]
        first_slot, tiles = (0, slots) if c < wide else (0 if ext else 2 * x, look + 2)
        parts = -(-tiles // 6)
        done = 0
        for part in range(parts):
            many = (tiles - done) // (parts - part)
            slot = first_slot + done
            done += many
            block = many * tok
            at = pl.ds(pl.multiple_of(slot * tok, tok), block)
            lat = lat_all[pl.ds(slot, many)].reshape(block, rank)
            low = lax.broadcasted_iota(jnp.int32, (block, NOPE), 1) < ROPE

            def up(kv, pair):
                cols = slice(pair * 2 * NOPE, (pair + 1) * 2 * NOPE)
                return jnp.dot(
                    lat, w[c, :, kv, :, cols].reshape(rank, 2 * NOPE),
                    preferred_element_type=jnp.float32,
                )

            for pair in range(pairs):
                k = up(0, pair)
                kaug[2 * pair, at, :NOPE] = k[:, :NOPE].astype(jnp.bfloat16)
                turned = pltpu.roll(k[:, NOPE:], ROPE, axis=1)
                kaug[2 * pair + 1, at, :NOPE] = jnp.where(low, 0.0, turned).astype(jnp.bfloat16)
                rope_last = kaug[2 * pair + 1, at, NOPE:].astype(jnp.float32)
                kaug[2 * pair + 1, at, NOPE:] = jnp.where(low, turned, rope_last).astype(
                    jnp.bfloat16
                )
            for pair in range(pairs):
                v = up(1, pair)
                for side in range(2):
                    begin = (2 * pair + side) * 2 * VDIM
                    vbuf[at, begin:begin + VDIM] = v[:, side * VDIM:(side + 1) * VDIM].astype(
                        jnp.bfloat16
                    )

    scale = LOG2E / math.sqrt(QK)

    def attend(c, tiles, then, ext):
        _, kaug, vbuf, bias, queries_in, given_out = ext_refs if ext else own_refs
        if not ext:
            queries_in, given_out = qbuf.at[c], obuf.at[c]

        def places(tile):
            place_of = tile if c < wide or ext else 2 * x + tile
            return place_of, pl.ds(pl.multiple_of(place_of * tok, tok), span)

        def scores(tile, h):
            begin = (h // 2) * 2 * QK + (h % 2) * NOPE
            return lax.dot_general(
                queries_in[tile, :, begin:begin + 2 * NOPE], kaug[h, places(tile)[1], :],
                (((1,), (1,)), ((), ())), preferred_element_type=jnp.float32,
            )

        def weights(tile, s):
            s = s * scale + bias[places(tile)[0]]
            peak = jnp.max(s, axis=1, keepdims=True)
            return jnp.exp2(s - peak).astype(jnp.bfloat16)

        def mix(tile, h, expo):
            both = jnp.dot(
                expo, vbuf[places(tile)[1], h * 2 * VDIM:(h + 1) * 2 * VDIM],
                preferred_element_type=jnp.float32,
            )
            given = (both[:, :VDIM] / both[:, VDIM:]).astype(jnp.bfloat16)
            given_out[tile, :, h * VDIM:(h + 1) * VDIM] = given

        items = [(tile, h) for tile in tiles for h in range(chunk_heads)]
        held = [scores(tile, h) for tile, h in items]
        expo = {}
        for i, (tile, h) in enumerate(items):
            expo[i] = weights(tile, held[i])
            if i > 0:
                mix(*items[i - 1], expo.pop(i - 1))
            if i == chunk_heads and c == last and not ext:
                then[0]()
        mix(*items[-1], expo.pop(len(items) - 1))
        if c != last or ext:
            then[0]()
        then[1]()

    def q_in(c):
        landed = qbuf.at[c] if c < wide else qbuf.at[c, pl.ds(0, 2)]
        pltpu.make_async_copy(landed, landed, q_sem.at[c]).wait()

    last = wide if cols else order[-1][0]

    def work_on(c):
        tiles = n_head if c < wide else 2

        def pair(j):
            def keep():
                who = head if c < wide else owner(c - wide, core)
                out[:, o_cols(who, c)] = obuf[c, tile_at(c, j + 1)]

            second_sent = o_copy(c, j + 1).start if j + 2 < tiles else keep
            if j == 0:
                with jax.named_scope(f"q_in{c}"):
                    q_in(c)
            with jax.named_scope(f"work{c}_{j}"):
                if j == 0:
                    project(c, False)
                attend(c, [tile_at(c, j), tile_at(c, j + 1)], (o_copy(c, j).start, second_sent), False)

        def ally_pair():
            arrive(q_ext, qe_sem)
            project(c, True)
            attend(c, [0, 1], (ext_out(0).start, ext_out(1).start), True)

        if cols and c > wide:
            return [
                (0.8, lambda: pl.when(inner)(lambda: pair(0))),
                (0.8, lambda: pl.when(inner)(ally_pair)),
            ]
        return [(0.8, functools.partial(pair, j)) for j in range(0, tiles, 2)]

    def column_plan():
        def only_inner(work):
            return lambda: pl.when(inner)(work)

        def only_outer(work):
            return lambda: pl.when(outer)(work)

        def ext_in():
            ext_done()
            rope_in(rope_ext, kaug_ext, look + 2)

        def back():
            pl.when(outer & (core == 0))(ext_give_back)

        def relay_back():
            pl.when(inner & (core == 0))(ext_relay_back)

        steps = {"r": ring_step, "z": z_take, "y": y_take}
        plan = PLAN
        todo = {
            "lat": lat_relay, "q1": lambda: start(q_copies(1)), "q2": lambda: start(q_copies(2)),
            "qx": only_outer(ext_queries), "back": back_relay, "done": lat_done,
            "rope": rope_own, "give": back, "own": only_outer(ext_give_own),
            "e3": only_outer(lambda: column_start(3)),
            "i3": only_inner(lambda: column_start(3)),
            "row": only_outer(row_take), "relay": only_inner(ext_relay), "pass": relay_back,
            "in": only_inner(ext_in),
        }
        waiting = []
        for step in plan:
            kind, rest = step[0], step[1:]
            with jax.named_scope(step):
                if step in todo:
                    todo[step]()
                elif kind == "b":
                    column_start(int(rest))
                elif kind == "w":
                    waiting += work_on(int(rest))
                else:
                    steps[kind](*map(int, rest))
            room = 1.8 if kind in "rzyw" else 0
            while waiting and room > 0:
                cost, work = waiting.pop(0)
                work()
                room -= cost
        for _, work in waiting:
            work()

    def ring_step(c, t):
        ring_take(c, t)
        if t < half:
            ring_send(c, t + 1)

    def ring_plan():
        chores = {
            (0, 1): [lat_relay],
            (1, 1): [lambda c=c: start(q_copies(c)) for c in range(1, min(2, wide))]
            + [lambda k=k: x_copy(k, 0).start() for k in range(1, xs)],
            (0, min(3, half - 1)): [back_relay],
        }
        chores.setdefault(order[order.index((0, half)) - 1], []).extend([lat_done, rope_own])
        chores.setdefault((wide, 1), []).extend(
            [lambda k=k: x_copy(k, 1).start() for k in range(1, xs)]
            + [lambda c=c: start(q_copies(c)) for c in range(2, wide)]
        )
        unsent, waiting, taken = order[2:], [], set()
        for c, t in order:
            with jax.named_scope(f"ring{c}_{t}"):
                ring_take(c, t)
            taken.add((c, t))
            while unsent:
                ahead, step = unsent[0]
                need = (ahead, step - 1) if step > 1 else holds.get(ahead)
                if need is not None and need not in taken:
                    break
                ring_send(*unsent.pop(0))
            for chore in chores.get((c, t), []):
                with jax.named_scope("chore"):
                    chore()
            if t == steps_of(c):
                waiting += work_on(c)
            room = 1.8
            while waiting and room > 0:
                cost, step = waiting.pop(0)
                step()
                room -= cost
        for _, step in waiting:
            step()

    if cols:
        column_plan()
    else:
        ring_plan()

    with jax.named_scope("last"):
        def outs(many):
            arrive(out.at[:, pl.ds(0, (wide * (n_head - 1) + many) * cw)], o_sem)

        if cols:
            pl.when(inner)(lambda: outs(xs))
            pl.when(outer)(lambda: outs(xs + 1))
        else:
            outs(xs)

    with jax.named_scope("sends"):
        arrive(obuf.at[pl.ds(0, wide), pl.ds(0, n_head - 1)], o_send.at[0])
        arrive(qbuf.at[pl.ds(0, wide), pl.ds(0, n_head - 1)], q_send.at[0])

        def local_sent(many):
            arrive(obuf.at[pl.ds(wide, many), pl.ds(0, 1)], o_send.at[1])
            arrive(qbuf.at[pl.ds(wide, many), pl.ds(0, 1)], q_send.at[1])

        if cols:
            arrive(w.at[0, pl.ds(0, n_seq - 1)], w_send.at[0])
            arrive(w.at[0, 0], x_send.at[0])

            def inner_sent():
                local_sent(2)
                arrive(w.at[pl.ds(0, 3), pl.ds(0, 6)], c_send.at[0])
                arrive(w.at[pl.ds(0, 2), pl.ds(0, 7)], c_send.at[1])
                arrive(obuf_ext, oe_send)

            def outer_sent():
                local_sent(1)
                arrive(w.at[pl.ds(0, 2), pl.ds(0, 5)], c_send.at[0])
                arrive(w.at[0, pl.ds(0, 7)], c_send.at[1])
                arrive(q_ext, qe_send)

            pl.when(inner)(inner_sent)
            pl.when(outer)(outer_sent)

            def ext_sent(index):
                arrive(lat_ext.at[0], ext_send.at[index, 0])
                arrive(rope_ext.at[0], ext_send.at[index, 1])

            ext_sent(0)
            pl.when(core == 0)(lambda: ext_sent(1))
        else:
            local_sent(xs)
            arrive(w.at[pl.ds(0, wide + 1), pl.ds(0, n_seq - 1)], w_send.at[0])
            arrive(w.at[pl.ds(wide + 1, xs - 1), pl.ds(0, n_seq - 2)], w_send.at[1])
            for k in range(1, xs):
                arrive(w.at[wide, pl.ds(0, 2)], x_send.at[k - 1])
        arrive(lat_all.at[pl.ds(0, 2 * xs - 1)], lat_send.at[0, 0])
        arrive(rope_all.at[pl.ds(0, 2 * xs - 1)], lat_send.at[0, 1])

        for i in range(look):
            @pl.when(back_side(i) & (seq < n_seq - 1))
            def _():
                for copy in back_out(i):
                    copy.wait_send()

            @pl.when(back_side(i) & (seq > 0))
            def _():
                for copy in back_mate(i):
                    copy.wait_send()


def shards(queries, latent, rope_keys, key_weight, value_weight, doc_lengths):
    n_seq, n_head = lax.axis_size("seq"), lax.axis_size("head")
    tok, rank = latent.shape
    rows = key_weight.shape[0]
    local_heads = key_weight.shape[1] // NOPE
    docs = doc_lengths.shape[0]
    slot_rows = n_seq * n_head * tok // docs
    look = 2 * -(-slot_rows // tok) - 1
    chunk_heads = min(4, local_heads)
    wide = local_heads // chunk_heads - 1
    xs = n_head // 2
    pieces = wide + xs
    slots, span, half = look + n_head, (look + 1) * tok, n_seq // 2
    cw, qw = chunk_heads * NOPE, chunk_heads * QK
    anywhere = pl.BlockSpec(memory_space=pl.ANY)
    dma = pltpu.SemaphoreType.DMA
    bf16 = jnp.bfloat16
    return pl.pallas_call(
        functools.partial(kernel, (n_seq, n_head, look, wide, chunk_heads)),
        out_shape=pltpu.VMEM((tok, n_head * local_heads * VDIM), bf16),
        in_specs=[anywhere] * 6,
        out_specs=pl.BlockSpec(memory_space=pltpu.VMEM),
        scratch_shapes=[
            pltpu.VMEM((slots, tok, rank), bf16),
            pltpu.VMEM((slots, ROPE, tok), bf16),
            pltpu.VMEM((pieces, n_seq, 2, rows, cw), bf16),
            pltpu.VMEM((pieces, n_head, tok, qw), bf16),
            pltpu.VMEM((chunk_heads, slots * tok, 2 * NOPE), bf16),
            pltpu.VMEM((slots * tok, 2 * cw), bf16),
            pltpu.VMEM((n_head, tok, span), jnp.float32),
            pltpu.VMEM((pieces, n_head, tok, cw), bf16),
            pltpu.SMEM((docs,), jnp.int32),
            pltpu.VMEM((look + 2, tok, rank), bf16),
            pltpu.VMEM((look + 2, ROPE, tok), bf16),
            pltpu.VMEM((2, tok, qw), bf16),
            pltpu.VMEM((chunk_heads, (look + 2) * tok, 2 * NOPE), bf16),
            pltpu.VMEM(((look + 2) * tok, 2 * cw), bf16),
            pltpu.VMEM((2, tok, span), jnp.float32),
            pltpu.VMEM((2, tok, cw), bf16),
            dma((4, 3)),
            dma((5,)),
            dma((2,)),
            dma((look + 2, 2)),
            dma((2, 2)),
            dma,
            dma,
            dma,
            dma,
            dma((slots, 2)),
            dma((1 + 2 * look, 2)),
            dma,
            dma((1 if (pieces, wide, half, look) == (5, 3, 4, 1) else pieces, half)),
            dma((2,)),
            dma((xs - 1,)),
            dma((xs - 1,)),
            dma((pieces,)),
            dma((2,)),
            dma,
            dma((2,)),
        ],
        compiler_params=pltpu.CompilerParams(collective_id=0, has_side_effects=True),
    )(queries, latent, rope_keys.T, key_weight, value_weight, doc_lengths)


def solution(mesh):
    placed = (
        P(("seq", "head"), None),
        P(("seq", "head"), None),
        P(("seq", "head"), None),
        P("seq", "head"),
        P("seq", "head"),
        P(),
    )
    return jax.shard_map(
        shards, mesh=mesh, in_specs=placed, out_specs=P(("seq", "head"), None), check_vma=False
    )
```

```python
import functools
import math

import jax
import jax.numpy as jnp
from jax import lax
from jax.experimental import pallas as pl
from jax.experimental.pallas import tpu as pltpu
from jax.sharding import PartitionSpec as P

NOPE = 128
ROPE = 64
VDIM = 128
QK = NOPE + ROPE
LOG2E = 1.4426950408889634

MESH = pl.DeviceIdType.MESH


PLAN = (
    "r01", "lat", "q1", "z11", "b4", "own", "z21", "q2", "r02", "z41", "z12", "back", "z22",
    "r03", "e3", "done", "rope", "give", "qx", "z42", "i3", "z13", "z23", "r04", "w0",
    "relay", "z31", "y1", "w1", "pass", "row", "z32", "y2", "w2", "y4", "in", "w4", "z33",
    "y3", "w3",
)


def ring_order(pieces, wide, steps_of):
    if (pieces, wide, steps_of(0)) == (5, 3, 4):
        steps = (1, 11, 2, 12, 3, 31, 21, 13, 4, 22, 14, 32, 41, 23, 42, 24, 33, 43, 34)
        return [divmod(step, 10) for step in steps], {4: (2, 2)}
    first = [0, wide] + list(range(1, wide))
    flight, later, order = [(c, 1) for c in first[:2]], first[2:] + list(range(wide + 1, pieces)), []
    while flight:
        c, t = flight.pop(0)
        order.append((c, t))
        if t < steps_of(c):
            flight.append((c, t + 1))
        if t >= steps_of(c) // 2 and later and len(flight) < 3:
            flight.append((later.pop(0), 1))
    holds = {}
    for c in range(wide + 1, pieces):
        at = order.index((c, 1))
        holds[c] = order[max(at - 2, order.index((wide, 1)))]
    return order, holds


def kernel(
    sizes, queries, latent, rope_keys, key_weight, value_weight, lengths_in, out,
    lat_all, w, qbuf, kaug, vbuf, bias, obuf, lengths,
    lat_ext, q_ext, kaug_ext, vbuf_ext, bias_ext, obuf_ext,
    z_recv, y_recv, c_send, ext_sem, ext_send, qe_sem, qe_send, oe_send,
    len_sem, lat_sem, lat_send, w_own, w_recv, w_send, x_send, x_recv, q_sem, q_send, o_sem, o_send,
):
    n_seq, n_head, look, wide, chunk_heads = sizes
    tok, rank = latent.shape
    half = n_seq // 2
    xs = n_head // 2
    slots = look + n_head
    folds = rank // tok
    fold_rows = ROPE // folds
    span = (look + 1) * tok
    cw = chunk_heads * NOPE
    qw = chunk_heads * QK
    pieces = wide + xs
    q_all, o_all = (wide + 1) * qw, (wide + 1) * cw
    seq, head = lax.axis_index("seq"), lax.axis_index("head")
    core, x = head % 2, head // 2
    mate = head + 1 - 2 * core

    odd = seq % 2
    place = (seq // 2) * (1 - odd) + (n_seq - 1 - seq // 2) * odd

    def at_place(where):
        where = (where + n_seq) % n_seq
        fold = where // half
        return 2 * where * (1 - fold) + (2 * (n_seq - 1 - where) + 1) * fold

    after, before = at_place(place + 1), at_place(place - 1)

    cols = (pieces, wide, half, look) == (5, 3, 4, 1)
    z, y = seq // 2, seq % 2
    inner = (z > 0) & (z < half - 1)
    outer = jnp.logical_not(inner)
    other, ally = seq + 1 - 2 * y, seq + 2 - 4 * (z % 2)

    sides = sorted({(n_head - look + i) % 2 for i in range(look)})
    helps = (core >= 0) if len(sides) > 1 else (core == sides[0])
    gives, takes = helps & (seq < n_seq - 1), helps & (seq > 0)

    barrier = pltpu.get_barrier_semaphore()

    def greet(to_seq, to_head):
        pl.semaphore_signal(barrier, inc=1, device_id=(to_seq, to_head), device_id_type=MESH)

    greet(after, head)
    greet(before, head)
    for k in range(1, n_head):
        greet(seq, (head + k) % n_head)

    if cols:
        greet(other, head)
        greet(ally, mate)

    @pl.when(gives)
    def _():
        greet(seq + 1, head)

    @pl.when(takes)
    def _():
        greet(seq - 1, head)

    def owner(k, side):
        return ((x + k) % xs) * 2 + side

    def q_cols(who, c):
        return pl.ds(pl.multiple_of(who * q_all + c * qw, 128), qw)

    def own_copies():
        for c in range(wide + 1):
            for kv, source in enumerate((key_weight, value_weight)):
                pltpu.make_async_copy(
                    source.at[:, pl.ds(c * cw, cw)], w.at[c, seq, kv], w_own
                ).start()
        mine = look + head
        pltpu.make_async_copy(latent, lat_all.at[mine, pl.ds(0, tok)], lat_sem.at[mine]).start()
        for a in range(folds):
            pltpu.make_async_copy(
                rope_keys.at[pl.ds(a * fold_rows, fold_rows)],
                lat_all.at[mine, pl.ds(tok, fold_rows), pl.ds(a * tok, tok)], lat_sem.at[mine],
            ).start()
        for c in range(wide):
            pltpu.make_async_copy(
                queries.at[:, q_cols(head, c)], qbuf.at[c, head], q_sem.at[c]
            ).start()
        for k in range(xs):
            mine_too = pltpu.make_async_copy(
                queries.at[:, q_cols(owner(k, core), wide)],
                qbuf.at[wide + k, core], q_sem.at[wide + k],
            )
            if cols and k > 0:
                pl.when(inner)(mine_too.start)
            else:
                mine_too.start()

    own_copies()
    pltpu.make_async_copy(lengths_in, lengths, len_sem).start()
    with jax.named_scope("barrier"):
        pl.semaphore_wait(
            barrier,
            n_head + 1 + 2 * cols + gives.astype(jnp.int32) + takes.astype(jnp.int32),
        )

    def lat_copies(index, slot, to, landing):
        return [
            pltpu.make_async_remote_copy(
                src_ref=lat_all.at[slot], dst_ref=lat_all.at[landing],
                send_sem=lat_send.at[index], recv_sem=lat_sem.at[landing],
                device_id=to, device_id_type=MESH,
            )
        ]

    def lat_wait(slot):
        pltpu.make_async_copy(lat_all.at[slot], lat_all.at[slot], lat_sem.at[slot]).wait()

    mine = look + head

    def lat_out():
        sent = [lat_copies(0, mine, (seq, owner(k, core)), mine) for k in range(1, xs)]
        return sent + [lat_copies(0, mine, (seq, mate), mine)]

    def lat_on(k):
        slot = look + owner(k, core)
        return lat_copies(0, slot, (seq, mate), slot)

    def back_out(i):
        return lat_copies(1 + i, n_head + i, (seq + 1, head), i)

    def back_mate(i):
        return lat_copies(1 + look + i, i, (seq, mate), i)

    def back_side(i):
        return core == (n_head - look + i) % 2

    def start(copies):
        for copy in copies:
            copy.start()

    def x_copy(k, near):
        rows_of = seq if near == 0 else before
        return pltpu.make_async_remote_copy(
            src_ref=w.at[wide, rows_of], dst_ref=w.at[wide + k, rows_of],
            send_sem=x_send.at[k - 1], recv_sem=x_recv.at[k - 1],
            device_id=(seq, owner(xs - k, core)), device_id_type=MESH,
        )

    def arrive(ref, sem):
        pltpu.make_async_copy(ref, ref, sem).wait()

    def steps_of(c):
        return half if c <= wide else half - 1

    def origin_at(c, t, way):
        return at_place(place - t - (c > wide)) if way == 0 else at_place(place + t)

    pairs = chunk_heads // 2

    def ring_copy(c, t, way):
        origin = origin_at(c, t - 1, way)
        block = w.at[c, origin, way] if t == half else w.at[c, origin]
        return pltpu.make_async_remote_copy(
            src_ref=block, dst_ref=block, send_sem=w_send.at[0 if c <= wide else 1],
            recv_sem=w_recv.at[c, t - 1],
            device_id=(after if way == 0 else before, head), device_id_type=MESH,
        )

    def ring_send(c, t):
        if t == 1 and c > wide:
            arrive(w.at[c, pl.ds(0, 2)], x_recv.at[c - wide - 1])
        for way in range(2):
            ring_copy(c, t, way).start()

    def ring_take(c, t):
        arrive(w.at[c, 0] if t == half else w.at[c, pl.ds(0, 2)], w_recv.at[c, t - 1])

    pairs = chunk_heads // 2

    def q_copies(c):
        if c < wide:
            routes = [((head + k) % n_head,) * 2 + (head,) for k in range(1, n_head)]
        else:
            routes = [(mate, owner(c - wide, 1 - core), core)]
        return [
            pltpu.make_async_remote_copy(
                src_ref=queries.at[:, q_cols(who, min(c, wide))], dst_ref=qbuf.at[c, slot],
                send_sem=q_send.at[0 if c < wide else 1], recv_sem=q_sem.at[c],
                device_id=(seq, peer), device_id_type=MESH,
            )
            for peer, who, slot in routes
        ]

    def tile_at(c, j):
        if c >= wide:
            return 1 - core if j == 0 else core
        if j < n_head - 2:
            return (2 * x + 2 + j) % n_head
        return mate if j == n_head - 2 else head

    def o_cols(who, c):
        return pl.ds(pl.multiple_of(who * o_all + min(c, wide) * cw, 128), cw)

    def o_copy(c, j):
        tile = tile_at(c, j)
        peer, who = (tile, head) if c < wide else (mate, owner(c - wide, core))
        return pltpu.make_async_remote_copy(
            src_ref=obuf.at[c, tile], dst_ref=out.at[:, o_cols(who, c)],
            send_sem=o_send.at[0 if c < wide else 1], recv_sem=o_sem,
            device_id=(seq, peer), device_id_type=MESH,
        )

    def z_copy(c, t, origin, up):
        block = w.at[c, 2 * origin + y]
        return pltpu.make_async_remote_copy(
            src_ref=block, dst_ref=block, send_sem=c_send.at[c // 3],
            recv_sem=z_recv.at[c - 1, t - 1],
            device_id=(seq + 2 * up, head), device_id_type=MESH,
        )

    def y_copy(c, t, origin):
        block = w.at[c, 2 * origin + y]
        return pltpu.make_async_remote_copy(
            src_ref=block, dst_ref=block, send_sem=c_send.at[c // 3],
            recv_sem=y_recv.at[4 if c == 3 and t == 0 else c - 1],
            device_id=(other, head), device_id_type=MESH,
        )

    def column_start(c):
        if c == 4:
            arrive(w.at[c, 0], x_recv.at[0])
        pl.when(z <= (half - 3 if c == 4 else half - 2))(z_copy(c, 1, z, 1).start)
        pl.when(z >= (2 if c == 4 else 1))(z_copy(c, 1, z, -1).start)
        if c == 4:
            pl.when(inner)(y_copy(c, 0, z).start)
        else:
            y_copy(c, 0, z).start()

    def z_take(c, t):
        one, two, sem = w.at[c, 0], w.at[c, pl.ds(0, 2)], z_recv.at[c - 1, t - 1]
        far = z + 2 - 4 * (z // 2)

        def first_inner():
            arrive(two, sem)
            pl.when(z <= (1 if c == 4 else half))(z_copy(c, 2, z - 1, 1).start)
            pl.when(z >= (2 if c == 4 else 0))(z_copy(c, 2, z + 1, -1).start)
            if c == 3:
                y_copy(c, 1, half - 1 - z).start()
            else:
                y_copy(c, 1, z - 1).start()
                y_copy(c, 1, z + 1).start()

        def first_outer():
            arrive(one, sem)
            y_copy(c, 1, z + 1 - 2 * (z % 2)).start()

        def second():
            arrive(one, sem)
            if c < 4:
                pl.when(z == 1)(z_copy(c, 3, far, -1).start)
                pl.when(z == 2)(z_copy(c, 3, far, 1).start)
            y_copy(c, 2, far).start()

        def third():
            arrive(one, sem)
            y_copy(c, 3, half - 1 - z).start()

        if t == 1:
            pl.when(inner)(first_inner)
            if c < 4:
                pl.when(outer)(first_outer)
        elif t == 2 and c == 4:
            pl.when(inner)(second)
        elif t == 2:
            second()
        elif c < 4:
            pl.when(outer)(third)

    def y_take(c):
        def whole():
            arrive(w.at[c, pl.ds(0, 4)], y_recv.at[c - 1])

        if c == 3:
            pl.when(inner)(lambda: arrive(w.at[c, 0], y_recv.at[4]))
            arrive(w.at[c, pl.ds(0, 3)], y_recv.at[c - 1])
        elif c == 4:
            pl.when(inner)(whole)
        else:
            whole()

    def row_on():
        block = w.at[3, other]
        return pltpu.make_async_remote_copy(
            src_ref=block, dst_ref=block, send_sem=c_send.at[1], recv_sem=y_recv.at[2],
            device_id=(ally, head), device_id_type=MESH,
        )

    def row_take():
        arrive(w.at[3, 0], y_recv.at[4])
        row_on().start()

    def ext_copies(index, source, slot, to):
        return [
            pltpu.make_async_remote_copy(
                src_ref=source, dst_ref=lat_ext.at[slot],
                send_sem=ext_send.at[index], recv_sem=ext_sem.at[slot],
                device_id=to, device_id_type=MESH,
            )
        ]

    def ext_wait(slot):
        arrive(lat_ext.at[slot], ext_sem.at[slot])

    def ext_give_own():
        start(ext_copies(0, lat_all.at[mine], 1 + core, (ally, head)))

    def ext_give_back():
        start(ext_copies(1, lat_all.at[2 * x], 0, (ally, head)))

    def ext_relay():
        ext_wait(1 + core)
        start(ext_copies(0, lat_ext.at[1 + core], 1 + core, (seq, mate)))

    def ext_relay_back():
        ext_wait(0)
        start(ext_copies(1, lat_ext.at[0], 0, (seq, mate)))

    def ext_done():
        ext_wait(2 - core)
        pl.when(core == 1)(lambda: ext_wait(0))

    def ext_queries():
        for side in range(2):
            pltpu.make_async_remote_copy(
                src_ref=queries.at[:, q_cols(owner(1, side), wide)], dst_ref=q_ext.at[core],
                send_sem=qe_send, recv_sem=qe_sem,
                device_id=(ally, 2 * x + side), device_id_type=MESH,
            ).start()

    def ext_out(tile):
        return pltpu.make_async_remote_copy(
            src_ref=obuf_ext.at[tile], dst_ref=out.at[:, o_cols(owner(1, core), wide)],
            send_sem=oe_send, recv_sem=o_sem,
            device_id=(ally, 2 * x + tile), device_id_type=MESH,
        )

    order, holds = ring_order(pieces, wide, steps_of)
    arrive(w.at[pl.ds(0, wide + 1), 0], w_own)
    lat_wait(mine)
    start([copy for copies in lat_out() for copy in copies])
    if cols:
        x_copy(1, 0).start()
    ring_send(*order[0])
    if cols:
        column_start(1)
        column_start(2)
    else:
        ring_send(*order[1])
    start(q_copies(0))
    for c in range(wide, pieces):
        if cols and c > wide:
            pl.when(inner)(lambda: start(q_copies(c)))
        else:
            start(q_copies(c))

    docs = lengths.shape[0]

    def mask_of(group, j):
        first = group * n_head * tok
        q_place = first + j * tok + lax.broadcasted_iota(jnp.int32, (tok, 1), 0)

        def document(d, state):
            begin, begun = state
            return begin + lengths[d], jnp.where(begin <= q_place, begin, begun)

        _, begun = lax.fori_loop(
            0, docs, document, (jnp.int32(0), jnp.zeros((tok, 1), jnp.int32)), unroll=True
        )
        k_place = first + (j - look) * tok + lax.broadcasted_iota(jnp.int32, (tok, span), 1)
        seen = (k_place >= begun) & (k_place <= q_place)
        return jnp.where(seen, 0.0, -jnp.inf)

    def mask_tile(j, carry):
        bias[j] = mask_of(seq, j)
        return carry

    def mask_ext(j, carry):
        bias_ext[j] = mask_of(ally, 2 * x + j)
        return carry

    with jax.named_scope("mask"):
        pltpu.make_async_copy(lengths_in, lengths, len_sem).wait()
        lax.fori_loop(0, n_head, mask_tile, 0)
        if cols:
            @pl.when(inner)
            def _():
                lax.fori_loop(0, 2, mask_ext, 0)
                for h in range(chunk_heads):
                    vbuf_ext[:, (2 * h + 1) * VDIM:(2 * h + 2) * VDIM] = jnp.ones(
                        ((look + 2) * tok, VDIM), jnp.bfloat16
                    )

        @pl.when(seq == 0)
        def _():
            lat_all[:look] = jnp.zeros((look, tok + fold_rows, rank), jnp.bfloat16)

        for h in range(chunk_heads):
            vbuf[:, (2 * h + 1) * VDIM:(2 * h + 2) * VDIM] = jnp.ones(
                (slots * tok, VDIM), jnp.bfloat16
            )

    def lat_relay():
        for k in range(1, xs):
            lat_wait(look + owner(k, core))
            start(lat_on(k))

        for i in range(look):
            @pl.when(back_side(i) & (seq < n_seq - 1))
            def _():
                start(back_out(i))

    def back_relay():
        for i in range(look):
            @pl.when(back_side(i) & (seq > 0))
            def _():
                lat_wait(i)
                start(back_mate(i))

    def lat_done():
        for k in range(xs):
            lat_wait(look + owner(k, 1 - core))
        for i in range(look):
            @pl.when(jnp.logical_not(back_side(i)) & (seq > 0))
            def _():
                lat_wait(i)

    def rope_in(held, augmented, count):
        first_half = lax.broadcasted_iota(jnp.int32, (tok, 2 * ROPE), 1) < ROPE

        def fill(slot, carry):
            rope = jnp.concatenate(
                [held[slot, tok:, a * tok:(a + 1) * tok].astype(jnp.float32) for a in range(folds)],
                axis=0,
            )
            twice = jnp.concatenate([rope, rope], axis=0).T
            at = pl.ds(pl.multiple_of(slot * tok, tok), tok)
            for h in range(chunk_heads):
                laid = jnp.where(first_half, twice, 0.0) if h % 2 == 0 else twice
                augmented[h, at, NOPE:] = laid.astype(jnp.bfloat16)
            return carry

        lax.fori_loop(0, count, fill, 0)

    def rope_own():
        rope_in(lat_all, kaug, slots)

    own_refs = (lat_all, kaug, vbuf, bias, qbuf, obuf)
    ext_refs = (lat_ext, kaug_ext, vbuf_ext, bias_ext, q_ext, obuf_ext)

    def project(c, ext):
        lat_all, kaug, vbuf = (ext_refs if ext else own_refs)[:3]
        first_slot, tiles = (0, slots) if c < wide else (0 if ext else 2 * x, look + 2)
        parts = -(-tiles // 6)
        done = 0
        for part in range(parts):
            many = (tiles - done) // (parts - part)
            slot = first_slot + done
            done += many
            block = many * tok
            at = pl.ds(pl.multiple_of(slot * tok, tok), block)
            lat = lat_all[pl.ds(slot, many), :tok].reshape(block, rank)
            low = lax.broadcasted_iota(jnp.int32, (block, NOPE), 1) < ROPE

            def up(kv, pair):
                cols = slice(pair * 2 * NOPE, (pair + 1) * 2 * NOPE)
                return jnp.dot(
                    lat, w[c, :, kv, :, cols].reshape(rank, 2 * NOPE),
                    preferred_element_type=jnp.float32,
                )

            for pair in range(pairs):
                k = up(0, pair)
                kaug[2 * pair, at, :NOPE] = k[:, :NOPE].astype(jnp.bfloat16)
                turned = pltpu.roll(k[:, NOPE:], ROPE, axis=1)
                kaug[2 * pair + 1, at, :NOPE] = jnp.where(low, 0.0, turned).astype(jnp.bfloat16)
                rope_last = kaug[2 * pair + 1, at, NOPE:].astype(jnp.float32)
                kaug[2 * pair + 1, at, NOPE:] = jnp.where(low, turned, rope_last).astype(
                    jnp.bfloat16
                )
            for pair in range(pairs):
                v = up(1, pair)
                for side in range(2):
                    begin = (2 * pair + side) * 2 * VDIM
                    vbuf[at, begin:begin + VDIM] = v[:, side * VDIM:(side + 1) * VDIM].astype(
                        jnp.bfloat16
                    )

    scale = LOG2E / math.sqrt(QK)

    def attend(c, tiles, then, ext):
        _, kaug, vbuf, bias, queries_in, given_out = ext_refs if ext else own_refs
        if not ext:
            queries_in, given_out = qbuf.at[c], obuf.at[c]

        def places(tile):
            place_of = tile if c < wide or ext else 2 * x + tile
            return place_of, pl.ds(pl.multiple_of(place_of * tok, tok), span)

        def scores(tile, h):
            begin = (h // 2) * 2 * QK + (h % 2) * NOPE
            return lax.dot_general(
                queries_in[tile, :, begin:begin + 2 * NOPE], kaug[h, places(tile)[1], :],
                (((1,), (1,)), ((), ())), preferred_element_type=jnp.float32,
            )

        def weights(tile, s):
            s = s * scale + bias[places(tile)[0]]
            peak = jnp.max(s, axis=1, keepdims=True)
            return jnp.exp2(s - peak).astype(jnp.bfloat16)

        def mix(tile, h, expo):
            both = jnp.dot(
                expo, vbuf[places(tile)[1], h * 2 * VDIM:(h + 1) * 2 * VDIM],
                preferred_element_type=jnp.float32,
            )
            given = (both[:, :VDIM] / both[:, VDIM:]).astype(jnp.bfloat16)
            given_out[tile, :, h * VDIM:(h + 1) * VDIM] = given

        items = [(tile, h) for tile in tiles for h in range(chunk_heads)]
        held = [scores(tile, h) for tile, h in items]
        expo = {}
        for i, (tile, h) in enumerate(items):
            expo[i] = weights(tile, held[i])
            if i > 0:
                mix(*items[i - 1], expo.pop(i - 1))
            if i == chunk_heads and c == last and not ext:
                then[0]()
        mix(*items[-1], expo.pop(len(items) - 1))
        if c != last or ext:
            then[0]()
        then[1]()

    def q_in(c):
        landed = qbuf.at[c] if c < wide else qbuf.at[c, pl.ds(0, 2)]
        pltpu.make_async_copy(landed, landed, q_sem.at[c]).wait()

    last = wide if cols else order[-1][0]

    def work_on(c):
        tiles = n_head if c < wide else 2

        def pair(j):
            def keep():
                who = head if c < wide else owner(c - wide, core)
                out[:, o_cols(who, c)] = obuf[c, tile_at(c, j + 1)]

            second_sent = o_copy(c, j + 1).start if j + 2 < tiles else keep
            if j == 0:
                with jax.named_scope(f"q_in{c}"):
                    q_in(c)
            with jax.named_scope(f"work{c}_{j}"):
                if j == 0:
                    project(c, False)
                attend(c, [tile_at(c, j), tile_at(c, j + 1)], (o_copy(c, j).start, second_sent), False)

        def ally_pair():
            arrive(q_ext, qe_sem)
            project(c, True)
            attend(c, [0, 1], (ext_out(0).start, ext_out(1).start), True)

        if cols and c > wide:
            return [
                (0.8, lambda: pl.when(inner)(lambda: pair(0))),
                (0.8, lambda: pl.when(inner)(ally_pair)),
            ]
        return [(0.8, functools.partial(pair, j)) for j in range(0, tiles, 2)]

    def column_plan():
        def only_inner(work):
            return lambda: pl.when(inner)(work)

        def only_outer(work):
            return lambda: pl.when(outer)(work)

        def ext_in():
            ext_done()
            rope_in(lat_ext, kaug_ext, look + 2)

        def back():
            pl.when(outer & (core == 0))(ext_give_back)

        def relay_back():
            pl.when(inner & (core == 0))(ext_relay_back)

        steps = {"r": ring_step, "z": z_take, "y": y_take}
        plan = PLAN
        todo = {
            "lat": lat_relay, "q1": lambda: start(q_copies(1)), "q2": lambda: start(q_copies(2)),
            "qx": only_outer(ext_queries), "back": back_relay, "done": lat_done,
            "rope": rope_own, "give": back, "own": only_outer(ext_give_own),
            "e3": only_outer(lambda: column_start(3)),
            "i3": only_inner(lambda: column_start(3)),
            "row": only_outer(row_take), "relay": only_inner(ext_relay), "pass": relay_back,
            "in": only_inner(ext_in),
        }
        waiting = []
        for step in plan:
            kind, rest = step[0], step[1:]
            with jax.named_scope(step):
                if step in todo:
                    todo[step]()
                elif kind == "b":
                    column_start(int(rest))
                elif kind == "w":
                    waiting += work_on(int(rest))
                else:
                    steps[kind](*map(int, rest))
            room = 1.8 if kind in "rzyw" else 0
            while waiting and room > 0:
                cost, work = waiting.pop(0)
                work()
                room -= cost
        for _, work in waiting:
            work()

    def ring_step(c, t):
        ring_take(c, t)
        if t < half:
            ring_send(c, t + 1)

    def ring_plan():
        chores = {
            (0, 1): [lat_relay],
            (1, 1): [lambda c=c: start(q_copies(c)) for c in range(1, min(2, wide))]
            + [lambda k=k: x_copy(k, 0).start() for k in range(1, xs)],
            (0, min(3, half - 1)): [back_relay],
        }
        chores.setdefault(order[order.index((0, half)) - 1], []).extend([lat_done, rope_own])
        chores.setdefault((wide, 1), []).extend(
            [lambda k=k: x_copy(k, 1).start() for k in range(1, xs)]
            + [lambda c=c: start(q_copies(c)) for c in range(2, wide)]
        )
        unsent, waiting, taken = order[2:], [], set()
        for c, t in order:
            with jax.named_scope(f"ring{c}_{t}"):
                ring_take(c, t)
            taken.add((c, t))
            while unsent:
                ahead, step = unsent[0]
                need = (ahead, step - 1) if step > 1 else holds.get(ahead)
                if need is not None and need not in taken:
                    break
                ring_send(*unsent.pop(0))
            for chore in chores.get((c, t), []):
                with jax.named_scope("chore"):
                    chore()
            if t == steps_of(c):
                waiting += work_on(c)
            room = 1.8
            while waiting and room > 0:
                cost, step = waiting.pop(0)
                step()
                room -= cost
        for _, step in waiting:
            step()

    if cols:
        column_plan()
    else:
        ring_plan()

    with jax.named_scope("last"):
        def outs(many):
            arrive(out.at[:, pl.ds(0, (wide * (n_head - 1) + many) * cw)], o_sem)

        if cols:
            pl.when(inner)(lambda: outs(xs))
            pl.when(outer)(lambda: outs(xs + 1))
        else:
            outs(xs)

    with jax.named_scope("sends"):
        arrive(obuf.at[pl.ds(0, wide), pl.ds(0, n_head - 1)], o_send.at[0])
        arrive(qbuf.at[pl.ds(0, wide), pl.ds(0, n_head - 1)], q_send.at[0])

        def local_sent(many):
            arrive(obuf.at[pl.ds(wide, many), pl.ds(0, 1)], o_send.at[1])
            arrive(qbuf.at[pl.ds(wide, many), pl.ds(0, 1)], q_send.at[1])

        if cols:
            arrive(w.at[0, pl.ds(0, n_seq - 1)], w_send.at[0])
            arrive(w.at[0, 0], x_send.at[0])

            def inner_sent():
                local_sent(2)
                arrive(w.at[pl.ds(0, 3), pl.ds(0, 6)], c_send.at[0])
                arrive(w.at[pl.ds(0, 2), pl.ds(0, 7)], c_send.at[1])
                arrive(obuf_ext, oe_send)

            def outer_sent():
                local_sent(1)
                arrive(w.at[pl.ds(0, 2), pl.ds(0, 5)], c_send.at[0])
                arrive(w.at[0, pl.ds(0, 7)], c_send.at[1])
                arrive(q_ext, qe_send)

            pl.when(inner)(inner_sent)
            pl.when(outer)(outer_sent)

            def ext_sent(index):
                arrive(lat_ext.at[0], ext_send.at[index])

            ext_sent(0)
            pl.when(core == 0)(lambda: ext_sent(1))
        else:
            local_sent(xs)
            arrive(w.at[pl.ds(0, wide + 1), pl.ds(0, n_seq - 1)], w_send.at[0])
            arrive(w.at[pl.ds(wide + 1, xs - 1), pl.ds(0, n_seq - 2)], w_send.at[1])
            for k in range(1, xs):
                arrive(w.at[wide, pl.ds(0, 2)], x_send.at[k - 1])
        arrive(lat_all.at[pl.ds(0, 2 * xs - 1)], lat_send.at[0])

        for i in range(look):
            @pl.when(back_side(i) & (seq < n_seq - 1))
            def _():
                for copy in back_out(i):
                    copy.wait_send()

            @pl.when(back_side(i) & (seq > 0))
            def _():
                for copy in back_mate(i):
                    copy.wait_send()


def shards(queries, latent, rope_keys, key_weight, value_weight, doc_lengths):
    n_seq, n_head = lax.axis_size("seq"), lax.axis_size("head")
    tok, rank = latent.shape
    rows = key_weight.shape[0]
    local_heads = key_weight.shape[1] // NOPE
    docs = doc_lengths.shape[0]
    slot_rows = n_seq * n_head * tok // docs
    look = 2 * -(-slot_rows // tok) - 1
    chunk_heads = min(4, local_heads)
    wide = local_heads // chunk_heads - 1
    xs = n_head // 2
    pieces = wide + xs
    slots, span, half = look + n_head, (look + 1) * tok, n_seq // 2
    cw, qw = chunk_heads * NOPE, chunk_heads * QK
    anywhere = pl.BlockSpec(memory_space=pl.ANY)
    dma = pltpu.SemaphoreType.DMA
    bf16 = jnp.bfloat16
    return pl.pallas_call(
        functools.partial(kernel, (n_seq, n_head, look, wide, chunk_heads)),
        out_shape=pltpu.VMEM((tok, n_head * local_heads * VDIM), bf16),
        in_specs=[anywhere] * 6,
        out_specs=pl.BlockSpec(memory_space=pltpu.VMEM),
        scratch_shapes=[
            pltpu.VMEM((slots, tok + ROPE * tok // rank, rank), bf16),
            pltpu.VMEM((pieces, n_seq, 2, rows, cw), bf16),
            pltpu.VMEM((pieces, n_head, tok, qw), bf16),
            pltpu.VMEM((chunk_heads, slots * tok, 2 * NOPE), bf16),
            pltpu.VMEM((slots * tok, 2 * cw), bf16),
            pltpu.VMEM((n_head, tok, span), jnp.float32),
            pltpu.VMEM((pieces, n_head, tok, cw), bf16),
            pltpu.SMEM((docs,), jnp.int32),
            pltpu.VMEM((look + 2, tok + ROPE * tok // rank, rank), bf16),
            pltpu.VMEM((2, tok, qw), bf16),
            pltpu.VMEM((chunk_heads, (look + 2) * tok, 2 * NOPE), bf16),
            pltpu.VMEM(((look + 2) * tok, 2 * cw), bf16),
            pltpu.VMEM((2, tok, span), jnp.float32),
            pltpu.VMEM((2, tok, cw), bf16),
            dma((4, 3)),
            dma((5,)),
            dma((2,)),
            dma((look + 2,)),
            dma((2,)),
            dma,
            dma,
            dma,
            dma,
            dma((slots,)),
            dma((1 + 2 * look,)),
            dma,
            dma((1 if (pieces, wide, half, look) == (5, 3, 4, 1) else pieces, half)),
            dma((2,)),
            dma((xs - 1,)),
            dma((xs - 1,)),
            dma((pieces,)),
            dma((2,)),
            dma,
            dma((2,)),
        ],
        compiler_params=pltpu.CompilerParams(collective_id=0, has_side_effects=True),
    )(queries, latent, rope_keys.T, key_weight, value_weight, doc_lengths)


def solution(mesh):
    placed = (
        P(("seq", "head"), None),
        P(("seq", "head"), None),
        P(("seq", "head"), None),
        P("seq", "head"),
        P("seq", "head"),
        P(),
    )
    return jax.shard_map(
        shards, mesh=mesh, in_specs=placed, out_specs=P(("seq", "head"), None), check_vma=False
    )
```

```python
import functools
import math

import jax
import jax.numpy as jnp
from jax import lax
from jax.experimental import pallas as pl
from jax.experimental.pallas import tpu as pltpu
from jax.sharding import PartitionSpec as P

NOPE = 128
ROPE = 64
VDIM = 128
QK = NOPE + ROPE
LOG2E = 1.4426950408889634

MESH = pl.DeviceIdType.MESH


PLAN = (
    "r01", "lat", "q1", "z11", "b4", "own", "z21", "q2", "r02", "z41", "z12", "back", "z22",
    "r03", "e3", "done", "rope", "give", "qx", "z42", "i3", "z13", "z23", "r04", "w0",
    "relay", "z31", "y1", "w1", "pass", "row", "z32", "y2", "w2", "y4", "in", "w4", "z33",
    "y3", "w3",
)


def ring_order(pieces, wide, steps_of):
    if (pieces, wide, steps_of(0)) == (5, 3, 4):
        steps = (1, 11, 2, 12, 3, 31, 21, 13, 4, 22, 14, 32, 41, 23, 42, 24, 33, 43, 34)
        return [divmod(step, 10) for step in steps], {4: (2, 2)}
    first = [0, wide] + list(range(1, wide))
    flight, later, order = [(c, 1) for c in first[:2]], first[2:] + list(range(wide + 1, pieces)), []
    while flight:
        c, t = flight.pop(0)
        order.append((c, t))
        if t < steps_of(c):
            flight.append((c, t + 1))
        if t >= steps_of(c) // 2 and later and len(flight) < 3:
            flight.append((later.pop(0), 1))
    holds = {}
    for c in range(wide + 1, pieces):
        at = order.index((c, 1))
        holds[c] = order[max(at - 2, order.index((wide, 1)))]
    return order, holds


def kernel(
    sizes, queries, latent, rope_keys, key_weight, value_weight, lengths_in, out,
    lat_all, w, qbuf, kaug, vbuf, bias, obuf, lengths,
    lat_ext, q_ext, kaug_ext, vbuf_ext, bias_ext, obuf_ext,
    z_recv, y_recv, c_send, ext_sem, ext_send, qe_sem, qe_send, oe_send,
    len_sem, lat_sem, lat_send, w_own, w_recv, w_send, x_send, x_recv, q_sem, q_send, o_sem, o_send,
):
    n_seq, n_head, look, wide, chunk_heads = sizes
    tok, rank = latent.shape
    half = n_seq // 2
    xs = n_head // 2
    slots = look + n_head
    folds = rank // tok
    fold_rows = ROPE // folds
    span = (look + 1) * tok
    cw = chunk_heads * NOPE
    qw = chunk_heads * QK
    pieces = wide + xs
    q_all, o_all = (wide + 1) * qw, (wide + 1) * cw
    seq, head = lax.axis_index("seq"), lax.axis_index("head")
    core, x = head % 2, head // 2
    mate = head + 1 - 2 * core

    odd = seq % 2
    place = (seq // 2) * (1 - odd) + (n_seq - 1 - seq // 2) * odd

    def at_place(where):
        where = (where + n_seq) % n_seq
        fold = where // half
        return 2 * where * (1 - fold) + (2 * (n_seq - 1 - where) + 1) * fold

    after, before = at_place(place + 1), at_place(place - 1)

    cols = (pieces, wide, half, look) == (5, 3, 4, 1)
    z, y = seq // 2, seq % 2
    inner = (z > 0) & (z < half - 1)
    outer = jnp.logical_not(inner)
    other, ally = seq + 1 - 2 * y, seq + 2 - 4 * (z % 2)

    sides = sorted({(n_head - look + i) % 2 for i in range(look)})
    helps = (core >= 0) if len(sides) > 1 else (core == sides[0])
    gives, takes = helps & (seq < n_seq - 1), helps & (seq > 0)

    barrier = pltpu.get_barrier_semaphore()

    def greet(to_seq, to_head):
        pl.semaphore_signal(barrier, inc=1, device_id=(to_seq, to_head), device_id_type=MESH)

    greet(after, head)
    greet(before, head)
    for k in range(1, n_head):
        greet(seq, (head + k) % n_head)

    if cols:
        greet(other, head)
        greet(ally, mate)

    @pl.when(gives)
    def _():
        greet(seq + 1, head)

    @pl.when(takes)
    def _():
        greet(seq - 1, head)

    def owner(k, side):
        return ((x + k) % xs) * 2 + side

    def q_cols(who, c):
        return pl.ds(pl.multiple_of(who * q_all + c * qw, 128), qw)

    def own_copies():
        for c in range(wide + 1):
            for kv, source in enumerate((key_weight, value_weight)):
                pltpu.make_async_copy(
                    source.at[:, pl.ds(c * cw, cw)], w.at[c, seq, kv], w_own
                ).start()
        mine = look + head
        pltpu.make_async_copy(latent, lat_all.at[mine, pl.ds(0, tok)], lat_sem.at[mine]).start()
        for a in range(folds):
            pltpu.make_async_copy(
                rope_keys.at[pl.ds(a * fold_rows, fold_rows)],
                lat_all.at[mine, pl.ds(tok, fold_rows), pl.ds(a * tok, tok)], lat_sem.at[mine],
            ).start()
        for c in range(wide):
            pltpu.make_async_copy(
                queries.at[:, q_cols(head, c)], qbuf.at[c, head], q_sem.at[c]
            ).start()
        for k in range(xs):
            mine_too = pltpu.make_async_copy(
                queries.at[:, q_cols(owner(k, core), wide)],
                qbuf.at[wide + k, core], q_sem.at[wide + k],
            )
            if cols and k > 0:
                pl.when(inner)(mine_too.start)
            else:
                mine_too.start()

    own_copies()
    pltpu.make_async_copy(lengths_in, lengths, len_sem).start()
    with jax.named_scope("barrier"):
        pl.semaphore_wait(
            barrier,
            n_head + 1 + 2 * cols + gives.astype(jnp.int32) + takes.astype(jnp.int32),
        )

    def lat_copies(index, slot, to, landing):
        return [
            pltpu.make_async_remote_copy(
                src_ref=lat_all.at[slot], dst_ref=lat_all.at[landing],
                send_sem=lat_send.at[index], recv_sem=lat_sem.at[landing],
                device_id=to, device_id_type=MESH,
            )
        ]

    def lat_wait(slot):
        pltpu.make_async_copy(lat_all.at[slot], lat_all.at[slot], lat_sem.at[slot]).wait()

    mine = look + head

    def lat_out():
        sent = [lat_copies(0, mine, (seq, owner(k, core)), mine) for k in range(1, xs)]
        return sent + [lat_copies(0, mine, (seq, mate), mine)]

    def lat_on(k):
        slot = look + owner(k, core)
        return lat_copies(0, slot, (seq, mate), slot)

    def back_out(i):
        return lat_copies(1 + i, n_head + i, (seq + 1, head), i)

    def back_mate(i):
        return lat_copies(1 + look + i, i, (seq, mate), i)

    def back_side(i):
        return core == (n_head - look + i) % 2

    def start(copies):
        for copy in copies:
            copy.start()

    def x_copy(k, near):
        rows_of = seq if near == 0 else before
        return pltpu.make_async_remote_copy(
            src_ref=w.at[wide, rows_of], dst_ref=w.at[wide + k, rows_of],
            send_sem=x_send.at[k - 1], recv_sem=x_recv.at[k - 1],
            device_id=(seq, owner(xs - k, core)), device_id_type=MESH,
        )

    def arrive(ref, sem):
        pltpu.make_async_copy(ref, ref, sem).wait()

    def steps_of(c):
        return half if c <= wide else half - 1

    def origin_at(c, t, way):
        return at_place(place - t - (c > wide)) if way == 0 else at_place(place + t)

    pairs = chunk_heads // 2

    def ring_copy(c, t, way):
        origin = origin_at(c, t - 1, way)
        block = w.at[c, origin, way] if t == half else w.at[c, origin]
        return pltpu.make_async_remote_copy(
            src_ref=block, dst_ref=block, send_sem=w_send.at[0 if c <= wide else 1],
            recv_sem=w_recv.at[c, t - 1],
            device_id=(after if way == 0 else before, head), device_id_type=MESH,
        )

    def ring_send(c, t):
        if t == 1 and c > wide:
            arrive(w.at[c, pl.ds(0, 2)], x_recv.at[c - wide - 1])
        for way in range(2):
            ring_copy(c, t, way).start()

    def ring_take(c, t):
        arrive(w.at[c, 0] if t == half else w.at[c, pl.ds(0, 2)], w_recv.at[c, t - 1])

    pairs = chunk_heads // 2

    def q_copies(c):
        if c < wide:
            routes = [((head + k) % n_head,) * 2 + (head,) for k in range(1, n_head)]
        else:
            routes = [(mate, owner(c - wide, 1 - core), core)]
        return [
            pltpu.make_async_remote_copy(
                src_ref=queries.at[:, q_cols(who, min(c, wide))], dst_ref=qbuf.at[c, slot],
                send_sem=q_send.at[0 if c < wide else 1], recv_sem=q_sem.at[c],
                device_id=(seq, peer), device_id_type=MESH,
            )
            for peer, who, slot in routes
        ]

    def tile_at(c, j):
        if c >= wide:
            return 1 - core if j == 0 else core
        if j < n_head - 2:
            return (2 * x + 2 + j) % n_head
        return mate if j == n_head - 2 else head

    def o_cols(who, c):
        return pl.ds(pl.multiple_of(who * o_all + min(c, wide) * cw, 128), cw)

    def o_copy(c, j):
        tile = tile_at(c, j)
        peer, who = (tile, head) if c < wide else (mate, owner(c - wide, core))
        return pltpu.make_async_remote_copy(
            src_ref=obuf.at[c, tile], dst_ref=out.at[:, o_cols(who, c)],
            send_sem=o_send.at[0 if c < wide else 1], recv_sem=o_sem,
            device_id=(seq, peer), device_id_type=MESH,
        )

    def z_copy(c, t, origin, up):
        block = w.at[c, 2 * origin + y]
        return pltpu.make_async_remote_copy(
            src_ref=block, dst_ref=block, send_sem=c_send.at[c // 3],
            recv_sem=z_recv.at[c - 1, t - 1],
            device_id=(seq + 2 * up, head), device_id_type=MESH,
        )

    def y_copy(c, t, origin):
        block = w.at[c, 2 * origin + y]
        return pltpu.make_async_remote_copy(
            src_ref=block, dst_ref=block, send_sem=c_send.at[c // 3],
            recv_sem=y_recv.at[4 if c == 3 and t == 0 else c - 1],
            device_id=(other, head), device_id_type=MESH,
        )

    def column_start(c):
        if c == 4:
            arrive(w.at[c, 0], x_recv.at[0])
        pl.when(z <= (half - 3 if c == 4 else half - 2))(z_copy(c, 1, z, 1).start)
        pl.when(z >= (2 if c == 4 else 1))(z_copy(c, 1, z, -1).start)
        if c == 4:
            pl.when(inner)(y_copy(c, 0, z).start)
        else:
            y_copy(c, 0, z).start()

    def z_take(c, t):
        one, two, sem = w.at[c, 0], w.at[c, pl.ds(0, 2)], z_recv.at[c - 1, t - 1]
        far = z + 2 - 4 * (z // 2)

        def first_inner():
            arrive(two, sem)
            pl.when(z <= (1 if c == 4 else half))(z_copy(c, 2, z - 1, 1).start)
            pl.when(z >= (2 if c == 4 else 0))(z_copy(c, 2, z + 1, -1).start)
            if c == 3:
                y_copy(c, 1, half - 1 - z).start()
            else:
                y_copy(c, 1, z - 1).start()
                y_copy(c, 1, z + 1).start()

        def first_outer():
            arrive(one, sem)
            y_copy(c, 1, z + 1 - 2 * (z % 2)).start()

        def second():
            arrive(one, sem)
            if c < 4:
                pl.when(z == 1)(z_copy(c, 3, far, -1).start)
                pl.when(z == 2)(z_copy(c, 3, far, 1).start)
            y_copy(c, 2, far).start()

        def third():
            arrive(one, sem)
            y_copy(c, 3, half - 1 - z).start()

        if t == 1:
            pl.when(inner)(first_inner)
            if c < 4:
                pl.when(outer)(first_outer)
        elif t == 2 and c == 4:
            pl.when(inner)(second)
        elif t == 2:
            second()
        elif c < 4:
            pl.when(outer)(third)

    def y_take(c):
        def whole():
            arrive(w.at[c, pl.ds(0, 4)], y_recv.at[c - 1])

        if c == 3:
            pl.when(inner)(lambda: arrive(w.at[c, 0], y_recv.at[4]))
            arrive(w.at[c, pl.ds(0, 3)], y_recv.at[c - 1])
        elif c == 4:
            pl.when(inner)(whole)
        else:
            whole()

    def row_on():
        block = w.at[3, other]
        return pltpu.make_async_remote_copy(
            src_ref=block, dst_ref=block, send_sem=c_send.at[1], recv_sem=y_recv.at[2],
            device_id=(ally, head), device_id_type=MESH,
        )

    def row_take():
        arrive(w.at[3, 0], y_recv.at[4])
        row_on().start()

    def ext_copies(index, source, slot, to):
        return [
            pltpu.make_async_remote_copy(
                src_ref=source, dst_ref=lat_ext.at[slot],
                send_sem=ext_send.at[index], recv_sem=ext_sem.at[slot],
                device_id=to, device_id_type=MESH,
            )
        ]

    def ext_wait(slot):
        arrive(lat_ext.at[slot], ext_sem.at[slot])

    def ext_give_own():
        start(ext_copies(0, lat_all.at[mine], 1 + core, (ally, head)))

    def ext_give_back():
        start(ext_copies(1, lat_all.at[2 * x], 0, (ally, head)))

    def ext_relay():
        ext_wait(1 + core)
        start(ext_copies(0, lat_ext.at[1 + core], 1 + core, (seq, mate)))

    def ext_relay_back():
        ext_wait(0)
        start(ext_copies(1, lat_ext.at[0], 0, (seq, mate)))

    def ext_done():
        ext_wait(2 - core)
        pl.when(core == 1)(lambda: ext_wait(0))

    def ext_queries():
        for side in range(2):
            pltpu.make_async_remote_copy(
                src_ref=queries.at[:, q_cols(owner(1, side), wide)], dst_ref=q_ext.at[core],
                send_sem=qe_send, recv_sem=qe_sem,
                device_id=(ally, 2 * x + side), device_id_type=MESH,
            ).start()

    def ext_out(tile):
        return pltpu.make_async_remote_copy(
            src_ref=obuf_ext.at[tile], dst_ref=out.at[:, o_cols(owner(1, core), wide)],
            send_sem=oe_send, recv_sem=o_sem,
            device_id=(ally, 2 * x + tile), device_id_type=MESH,
        )

    order, holds = ring_order(pieces, wide, steps_of)
    lat_wait(mine)
    start([copy for copies in lat_out() for copy in copies])
    arrive(w.at[pl.ds(0, wide + 1), 0], w_own)
    if cols:
        x_copy(1, 0).start()
    ring_send(*order[0])
    if cols:
        column_start(1)
        column_start(2)
    else:
        ring_send(*order[1])
    start(q_copies(0))
    for c in range(wide, pieces):
        if cols and c > wide:
            pl.when(inner)(lambda: start(q_copies(c)))
        else:
            start(q_copies(c))

    docs = lengths.shape[0]

    def mask_of(group, j):
        first = group * n_head * tok
        q_place = first + j * tok + lax.broadcasted_iota(jnp.int32, (tok, 1), 0)

        def document(d, state):
            begin, begun = state
            return begin + lengths[d], jnp.where(begin <= q_place, begin, begun)

        _, begun = lax.fori_loop(
            0, docs, document, (jnp.int32(0), jnp.zeros((tok, 1), jnp.int32)), unroll=True
        )
        k_place = first + (j - look) * tok + lax.broadcasted_iota(jnp.int32, (tok, span), 1)
        seen = (k_place >= begun) & (k_place <= q_place)
        return jnp.where(seen, 0.0, -jnp.inf)

    def mask_tile(j, carry):
        bias[j] = mask_of(seq, j)
        return carry

    def mask_ext(j, carry):
        bias_ext[j] = mask_of(ally, 2 * x + j)
        return carry

    with jax.named_scope("mask"):
        pltpu.make_async_copy(lengths_in, lengths, len_sem).wait()
        lax.fori_loop(0, n_head, mask_tile, 0)
        if cols:
            @pl.when(inner)
            def _():
                lax.fori_loop(0, 2, mask_ext, 0)
                for h in range(chunk_heads):
                    vbuf_ext[:, (2 * h + 1) * VDIM:(2 * h + 2) * VDIM] = jnp.ones(
                        ((look + 2) * tok, VDIM), jnp.bfloat16
                    )

        @pl.when(seq == 0)
        def _():
            lat_all[:look] = jnp.zeros((look, tok + fold_rows, rank), jnp.bfloat16)

        for h in range(chunk_heads):
            vbuf[:, (2 * h + 1) * VDIM:(2 * h + 2) * VDIM] = jnp.ones(
                (slots * tok, VDIM), jnp.bfloat16
            )

    def lat_relay():
        for k in range(1, xs):
            lat_wait(look + owner(k, core))
            start(lat_on(k))

        for i in range(look):
            @pl.when(back_side(i) & (seq < n_seq - 1))
            def _():
                start(back_out(i))

    def back_relay():
        for i in range(look):
            @pl.when(back_side(i) & (seq > 0))
            def _():
                lat_wait(i)
                start(back_mate(i))

    def lat_done():
        for k in range(xs):
            lat_wait(look + owner(k, 1 - core))
        for i in range(look):
            @pl.when(jnp.logical_not(back_side(i)) & (seq > 0))
            def _():
                lat_wait(i)

    def rope_in(held, augmented, count):
        first_half = lax.broadcasted_iota(jnp.int32, (tok, 2 * ROPE), 1) < ROPE

        def fill(slot, carry):
            rope = jnp.concatenate(
                [held[slot, tok:, a * tok:(a + 1) * tok].astype(jnp.float32) for a in range(folds)],
                axis=0,
            )
            twice = jnp.concatenate([rope, rope], axis=0).T
            at = pl.ds(pl.multiple_of(slot * tok, tok), tok)
            for h in range(chunk_heads):
                laid = jnp.where(first_half, twice, 0.0) if h % 2 == 0 else twice
                augmented[h, at, NOPE:] = laid.astype(jnp.bfloat16)
            return carry

        lax.fori_loop(0, count, fill, 0)

    def rope_own():
        rope_in(lat_all, kaug, slots)

    own_refs = (lat_all, kaug, vbuf, bias, qbuf, obuf)
    ext_refs = (lat_ext, kaug_ext, vbuf_ext, bias_ext, q_ext, obuf_ext)

    def project(c, ext):
        lat_all, kaug, vbuf = (ext_refs if ext else own_refs)[:3]
        first_slot, tiles = (0, slots) if c < wide else (0 if ext else 2 * x, look + 2)
        parts = -(-tiles // 6)
        done = 0
        for part in range(parts):
            many = (tiles - done) // (parts - part)
            slot = first_slot + done
            done += many
            block = many * tok
            at = pl.ds(pl.multiple_of(slot * tok, tok), block)
            lat = lat_all[pl.ds(slot, many), :tok].reshape(block, rank)
            low = lax.broadcasted_iota(jnp.int32, (block, NOPE), 1) < ROPE

            def up(kv, pair):
                cols = slice(pair * 2 * NOPE, (pair + 1) * 2 * NOPE)
                return jnp.dot(
                    lat, w[c, :, kv, :, cols].reshape(rank, 2 * NOPE),
                    preferred_element_type=jnp.float32,
                )

            for pair in range(pairs):
                k = up(0, pair)
                kaug[2 * pair, at, :NOPE] = k[:, :NOPE].astype(jnp.bfloat16)
                turned = pltpu.roll(k[:, NOPE:], ROPE, axis=1)
                kaug[2 * pair + 1, at, :NOPE] = jnp.where(low, 0.0, turned).astype(jnp.bfloat16)
                rope_last = kaug[2 * pair + 1, at, NOPE:].astype(jnp.float32)
                kaug[2 * pair + 1, at, NOPE:] = jnp.where(low, turned, rope_last).astype(
                    jnp.bfloat16
                )
            for pair in range(pairs):
                v = up(1, pair)
                for side in range(2):
                    begin = (2 * pair + side) * 2 * VDIM
                    vbuf[at, begin:begin + VDIM] = v[:, side * VDIM:(side + 1) * VDIM].astype(
                        jnp.bfloat16
                    )

    scale = LOG2E / math.sqrt(QK)

    def attend(c, tiles, then, ext):
        _, kaug, vbuf, bias, queries_in, given_out = ext_refs if ext else own_refs
        if not ext:
            queries_in, given_out = qbuf.at[c], obuf.at[c]

        def places(tile):
            place_of = tile if c < wide or ext else 2 * x + tile
            return place_of, pl.ds(pl.multiple_of(place_of * tok, tok), span)

        def scores(tile, h):
            begin = (h // 2) * 2 * QK + (h % 2) * NOPE
            return lax.dot_general(
                queries_in[tile, :, begin:begin + 2 * NOPE], kaug[h, places(tile)[1], :],
                (((1,), (1,)), ((), ())), preferred_element_type=jnp.float32,
            )

        def weights(tile, s):
            s = s * scale + bias[places(tile)[0]]
            peak = jnp.max(s, axis=1, keepdims=True)
            return jnp.exp2(s - peak).astype(jnp.bfloat16)

        def mix(tile, h, expo):
            both = jnp.dot(
                expo, vbuf[places(tile)[1], h * 2 * VDIM:(h + 1) * 2 * VDIM],
                preferred_element_type=jnp.float32,
            )
            given = (both[:, :VDIM] / both[:, VDIM:]).astype(jnp.bfloat16)
            given_out[tile, :, h * VDIM:(h + 1) * VDIM] = given

        items = [(tile, h) for tile in tiles for h in range(chunk_heads)]
        held = [scores(tile, h) for tile, h in items]
        expo = {}
        for i, (tile, h) in enumerate(items):
            expo[i] = weights(tile, held[i])
            if i > 0:
                mix(*items[i - 1], expo.pop(i - 1))
            if i == chunk_heads and c == last and not ext:
                then[0]()
        mix(*items[-1], expo.pop(len(items) - 1))
        if c != last or ext:
            then[0]()
        then[1]()

    def q_in(c):
        landed = qbuf.at[c] if c < wide else qbuf.at[c, pl.ds(0, 2)]
        pltpu.make_async_copy(landed, landed, q_sem.at[c]).wait()

    last = wide if cols else order[-1][0]

    def work_on(c):
        tiles = n_head if c < wide else 2

        def pair(j):
            def keep():
                who = head if c < wide else owner(c - wide, core)
                out[:, o_cols(who, c)] = obuf[c, tile_at(c, j + 1)]

            second_sent = o_copy(c, j + 1).start if j + 2 < tiles else keep
            if j == 0:
                with jax.named_scope(f"q_in{c}"):
                    q_in(c)
            with jax.named_scope(f"work{c}_{j}"):
                if j == 0:
                    project(c, False)
                attend(c, [tile_at(c, j), tile_at(c, j + 1)], (o_copy(c, j).start, second_sent), False)

        def ally_pair():
            arrive(q_ext, qe_sem)
            project(c, True)
            attend(c, [0, 1], (ext_out(0).start, ext_out(1).start), True)

        if cols and c > wide:
            return [
                (0.8, lambda: pl.when(inner)(lambda: pair(0))),
                (0.8, lambda: pl.when(inner)(ally_pair)),
            ]
        return [(0.8, functools.partial(pair, j)) for j in range(0, tiles, 2)]

    def column_plan():
        def only_inner(work):
            return lambda: pl.when(inner)(work)

        def only_outer(work):
            return lambda: pl.when(outer)(work)

        def ext_in():
            ext_done()
            rope_in(lat_ext, kaug_ext, look + 2)

        def back():
            pl.when(outer & (core == 0))(ext_give_back)

        def relay_back():
            pl.when(inner & (core == 0))(ext_relay_back)

        steps = {"r": ring_step, "z": z_take, "y": y_take}
        plan = PLAN
        todo = {
            "lat": lat_relay, "q1": lambda: start(q_copies(1)), "q2": lambda: start(q_copies(2)),
            "qx": only_outer(ext_queries), "back": back_relay, "done": lat_done,
            "rope": rope_own, "give": back, "own": only_outer(ext_give_own),
            "e3": only_outer(lambda: column_start(3)),
            "i3": only_inner(lambda: column_start(3)),
            "row": only_outer(row_take), "relay": only_inner(ext_relay), "pass": relay_back,
            "in": only_inner(ext_in),
        }
        waiting = []
        for step in plan:
            kind, rest = step[0], step[1:]
            with jax.named_scope(step):
                if step in todo:
                    todo[step]()
                elif kind == "b":
                    column_start(int(rest))
                elif kind == "w":
                    waiting += work_on(int(rest))
                else:
                    steps[kind](*map(int, rest))
            room = 1.8 if kind in "rzyw" else 0
            while waiting and room > 0:
                cost, work = waiting.pop(0)
                work()
                room -= cost
        for _, work in waiting:
            work()

    def ring_step(c, t):
        ring_take(c, t)
        if t < half:
            ring_send(c, t + 1)

    def ring_plan():
        chores = {
            (0, 1): [lat_relay],
            (1, 1): [lambda c=c: start(q_copies(c)) for c in range(1, min(2, wide))]
            + [lambda k=k: x_copy(k, 0).start() for k in range(1, xs)],
            (0, min(3, half - 1)): [back_relay],
        }
        chores.setdefault(order[order.index((0, half)) - 1], []).extend([lat_done, rope_own])
        chores.setdefault((wide, 1), []).extend(
            [lambda k=k: x_copy(k, 1).start() for k in range(1, xs)]
            + [lambda c=c: start(q_copies(c)) for c in range(2, wide)]
        )
        unsent, waiting, taken = order[2:], [], set()
        for c, t in order:
            with jax.named_scope(f"ring{c}_{t}"):
                ring_take(c, t)
            taken.add((c, t))
            while unsent:
                ahead, step = unsent[0]
                need = (ahead, step - 1) if step > 1 else holds.get(ahead)
                if need is not None and need not in taken:
                    break
                ring_send(*unsent.pop(0))
            for chore in chores.get((c, t), []):
                with jax.named_scope("chore"):
                    chore()
            if t == steps_of(c):
                waiting += work_on(c)
            room = 1.8
            while waiting and room > 0:
                cost, step = waiting.pop(0)
                step()
                room -= cost
        for _, step in waiting:
            step()

    if cols:
        column_plan()
    else:
        ring_plan()

    with jax.named_scope("last"):
        def outs(many):
            arrive(out.at[:, pl.ds(0, (wide * (n_head - 1) + many) * cw)], o_sem)

        if cols:
            pl.when(inner)(lambda: outs(xs))
            pl.when(outer)(lambda: outs(xs + 1))
        else:
            outs(xs)

    with jax.named_scope("sends"):
        arrive(obuf.at[pl.ds(0, wide), pl.ds(0, n_head - 1)], o_send.at[0])
        arrive(qbuf.at[pl.ds(0, wide), pl.ds(0, n_head - 1)], q_send.at[0])

        def local_sent(many):
            arrive(obuf.at[pl.ds(wide, many), pl.ds(0, 1)], o_send.at[1])
            arrive(qbuf.at[pl.ds(wide, many), pl.ds(0, 1)], q_send.at[1])

        if cols:
            arrive(w.at[0, pl.ds(0, n_seq - 1)], w_send.at[0])
            arrive(w.at[0, 0], x_send.at[0])

            def inner_sent():
                local_sent(2)
                arrive(w.at[pl.ds(0, 3), pl.ds(0, 6)], c_send.at[0])
                arrive(w.at[pl.ds(0, 2), pl.ds(0, 7)], c_send.at[1])
                arrive(obuf_ext, oe_send)

            def outer_sent():
                local_sent(1)
                arrive(w.at[pl.ds(0, 2), pl.ds(0, 5)], c_send.at[0])
                arrive(w.at[0, pl.ds(0, 7)], c_send.at[1])
                arrive(q_ext, qe_send)

            pl.when(inner)(inner_sent)
            pl.when(outer)(outer_sent)

            def ext_sent(index):
                arrive(lat_ext.at[0], ext_send.at[index])

            ext_sent(0)
            pl.when(core == 0)(lambda: ext_sent(1))
        else:
            local_sent(xs)
            arrive(w.at[pl.ds(0, wide + 1), pl.ds(0, n_seq - 1)], w_send.at[0])
            arrive(w.at[pl.ds(wide + 1, xs - 1), pl.ds(0, n_seq - 2)], w_send.at[1])
            for k in range(1, xs):
                arrive(w.at[wide, pl.ds(0, 2)], x_send.at[k - 1])
        arrive(lat_all.at[pl.ds(0, 2 * xs - 1)], lat_send.at[0])

        for i in range(look):
            @pl.when(back_side(i) & (seq < n_seq - 1))
            def _():
                for copy in back_out(i):
                    copy.wait_send()

            @pl.when(back_side(i) & (seq > 0))
            def _():
                for copy in back_mate(i):
                    copy.wait_send()


def shards(queries, latent, rope_keys, key_weight, value_weight, doc_lengths):
    n_seq, n_head = lax.axis_size("seq"), lax.axis_size("head")
    tok, rank = latent.shape
    rows = key_weight.shape[0]
    local_heads = key_weight.shape[1] // NOPE
    docs = doc_lengths.shape[0]
    slot_rows = n_seq * n_head * tok // docs
    look = 2 * -(-slot_rows // tok) - 1
    chunk_heads = min(4, local_heads)
    wide = local_heads // chunk_heads - 1
    xs = n_head // 2
    pieces = wide + xs
    slots, span, half = look + n_head, (look + 1) * tok, n_seq // 2
    cw, qw = chunk_heads * NOPE, chunk_heads * QK
    anywhere = pl.BlockSpec(memory_space=pl.ANY)
    dma = pltpu.SemaphoreType.DMA
    bf16 = jnp.bfloat16
    return pl.pallas_call(
        functools.partial(kernel, (n_seq, n_head, look, wide, chunk_heads)),
        out_shape=pltpu.VMEM((tok, n_head * local_heads * VDIM), bf16),
        in_specs=[anywhere] * 6,
        out_specs=pl.BlockSpec(memory_space=pltpu.VMEM),
        scratch_shapes=[
            pltpu.VMEM((slots, tok + ROPE * tok // rank, rank), bf16),
            pltpu.VMEM((pieces, n_seq, 2, rows, cw), bf16),
            pltpu.VMEM((pieces, n_head, tok, qw), bf16),
            pltpu.VMEM((chunk_heads, slots * tok, 2 * NOPE), bf16),
            pltpu.VMEM((slots * tok, 2 * cw), bf16),
            pltpu.VMEM((n_head, tok, span), jnp.float32),
            pltpu.VMEM((pieces, n_head, tok, cw), bf16),
            pltpu.SMEM((docs,), jnp.int32),
            pltpu.VMEM((look + 2, tok + ROPE * tok // rank, rank), bf16),
            pltpu.VMEM((2, tok, qw), bf16),
            pltpu.VMEM((chunk_heads, (look + 2) * tok, 2 * NOPE), bf16),
            pltpu.VMEM(((look + 2) * tok, 2 * cw), bf16),
            pltpu.VMEM((2, tok, span), jnp.float32),
            pltpu.VMEM((2, tok, cw), bf16),
            dma((4, 3)),
            dma((5,)),
            dma((2,)),
            dma((look + 2,)),
            dma((2,)),
            dma,
            dma,
            dma,
            dma,
            dma((slots,)),
            dma((1 + 2 * look,)),
            dma,
            dma((1 if (pieces, wide, half, look) == (5, 3, 4, 1) else pieces, half)),
            dma((2,)),
            dma((xs - 1,)),
            dma((xs - 1,)),
            dma((pieces,)),
            dma((2,)),
            dma,
            dma((2,)),
        ],
        compiler_params=pltpu.CompilerParams(collective_id=0, has_side_effects=True),
    )(queries, latent, rope_keys.T, key_weight, value_weight, doc_lengths)


def solution(mesh):
    placed = (
        P(("seq", "head"), None),
        P(("seq", "head"), None),
        P(("seq", "head"), None),
        P("seq", "head"),
        P("seq", "head"),
        P(),
    )
    return jax.shard_map(
        shards, mesh=mesh, in_specs=placed, out_specs=P(("seq", "head"), None), check_vma=False
    )
```
